256 devices in a mesh: gx: 4 (over y), gy: 16 (over z, core), gz: 4 (over x).
Axes of the slice: x: 4, y: 4, z: 8, core: 2. Of those that a mesh axis runs over, the one named last changes fastest.
Arguments:
- initial: float32 [256, 512, 1024], P('gx', 'gy', 'gz'), may hold values from -6 to 6
- right_side: float32 [256, 512, 1024], P('gx', 'gy', 'gz'), may hold values from -12 to 12
- shift_field: float32 [256, 512, 1024], P('gx', 'gy', 'gz'), may hold values from 0.5 to 8
Outputs:
- relaxed: float32 [256, 512, 1024], P('gx', 'gy', 'gz')
The draws below stay inside these ranges and needn't reach their ends.
All inputs are finite; a program needn't handle non-finite values.
Results may differ from the reference program's by a relative error of at most 0.00002.
Values sent between devices are 32-bit elements; how exact they have to be, the bound alone decides.
No kernel may reach another device: no remote copies, remote signals or barrier semaphores. Data moves between devices by JAX's collectives and lax.ppermute only.
A program may use at most 128 MiB of HBM per device.

```python
import math
import jax
import jax.numpy as jnp

SWEEPS = 4
NX = 256
NY = 512
NZ = 1024


def levels(stream_key, extent, cuts, least, high):
    def one(position, parts):
        heights = jax.random.uniform(jax.random.fold_in(jax.random.fold_in(stream_key, 6), position), (parts,), jnp.float32, least / len(cuts), high / len(cuts))
        return jnp.repeat(jnp.exp(heights), extent[position] // parts).reshape((-1,) + (1,) * (len(extent) - position - 1))

    gain = one(*cuts[0])
    for cut in cuts[1:]:
        gain = gain * one(*cut)
    return gain


def centred(stream_key, extent, scale, limit, pieces=(), held_as=jnp.bfloat16):
    array = scale * jax.random.normal(stream_key, extent, jnp.float32)
    if pieces:
        array = array * levels(stream_key, extent, pieces, -0.22, 0.18)
    return jnp.clip(array, -limit, limit).astype(held_as)


def setup_inputs(seed: int = 0) -> dict:
    keys = jax.random.split(jax.random.key(seed), 4)
    initial = centred(keys[0], (NX, NY, NZ), 1.0, 6.0, ((0, 4), (1, 16), (2, 4)), jnp.float32)
    right_side = centred(keys[1], (NX, NY, NZ), 2.0, 12.0, ((0, 4), (1, 16), (2, 4)), jnp.float32)
    shift_field = jnp.clip(jnp.exp(math.log(8.0) - 2.7725887 * jax.random.uniform(keys[2], (NX, NY, NZ), jnp.float32) ** levels(keys[2], (NX, NY, NZ), ((0, 4), (1, 16), (2, 4)), -0.2, 0.2)), 0.5, 8.0)
    return dict(initial=initial, right_side=right_side, shift_field=shift_field)


relax_weight = 0.8


def neighbours(field):
    total = jnp.roll(field, 1, 0) + jnp.roll(field, -1, 0)
    total = total + jnp.roll(field, 1, 1) + jnp.roll(field, -1, 1)
    total = total + jnp.roll(field, 1, 2) + jnp.roll(field, -1, 2)
    return total


def reference(initial, right_side, shift_field):
    diagonal = 6.0 + shift_field
    relaxed = initial
    for sweep in range(SWEEPS):
        beside = neighbours(relaxed)
        relaxed = relaxed + relax_weight * (right_side - (diagonal * relaxed - beside)) / diagonal
    return relaxed
```

```python
import functools

import jax
import jax.numpy as jnp
from jax import lax
from jax.experimental import pallas as pl
from jax.experimental.pallas import tpu as pltpu
from jax.sharding import PartitionSpec as P

SWEEPS = 4
WEIGHT = 0.8
UNROLL = 4
VMEM = pl.BlockSpec(memory_space=pltpu.VMEM)


def call(kernel, outs, operands, flops):
    return pl.pallas_call(
        kernel,
        out_shape=[jax.ShapeDtypeStruct(s, jnp.float32) for s in outs],
        in_specs=[VMEM] * len(operands),
        out_specs=[VMEM] * len(outs),
        compiler_params=pltpu.CompilerParams(vmem_limit_bytes=20 * 2**20),
        cost_estimate=pl.CostEstimate(flops=flops, bytes_accessed=2**22, transcendentals=0),
    )(*operands)


def put_faces(x, plane, lanes, y_low, y_high):
    ny, nz = plane.shape
    y_low[pl.ds(x, 1), :] = plane[0:1, :]
    y_high[pl.ds(x, 1), :] = plane[ny - 1 : ny, :]


def packed(x, column, total, lanes):
    return jnp.where(lanes == x, jnp.broadcast_to(column, total.shape), total)


def pack_kernel(u_ref, x_low, x_high, y_low, y_high, z_low, z_high):
    nx, ny, nz = u_ref.shape
    lanes = lax.broadcasted_iota(jnp.int32, (ny, 128), 1)
    x_low[...] = u_ref[0]
    x_high[...] = u_ref[nx - 1]

    def body(i, totals):
        low, high = totals
        for j in range(UNROLL):
            x = i * UNROLL + j
            plane = u_ref[x]
            put_faces(x, plane, lanes, y_low, y_high)
            low = packed(x, plane[:, 0:1], low, lanes)
            high = packed(x, plane[:, nz - 1 : nz], high, lanes)
        return low, high

    zero = jnp.zeros((ny, 128), jnp.float32)
    low, high = lax.fori_loop(0, nx // UNROLL, body, (zero, zero))
    z_low[...] = low
    z_high[...] = high


def weight_kernel(shift_ref, w_ref):
    def body(i, c):
        w_ref[i] = WEIGHT / (6.0 + shift_ref[i])
        return c

    lax.fori_loop(0, shift_ref.shape[0], body, 0, unroll=4)


def sweep_kernel(last, u_ref, rhs_ref, w_ref, xl, xh, yl, yh, zl, zh, new_ref, *faces):
    nx, ny, nz = u_ref.shape
    lanes = lax.broadcasted_iota(jnp.int32, (ny, 128), 1)
    zlane = lax.broadcasted_iota(jnp.int32, (ny, nz), 1)
    rows = lax.broadcasted_iota(jnp.int32, (ny, nz), 0)

    def update(x, below, here, above, totals):
        beside = below + above
        down = jnp.where(rows == 0, yl[pl.ds(x, 1), :], pltpu.roll(here, 1, 0))
        up = jnp.where(rows == ny - 1, yh[pl.ds(x, 1), :], pltpu.roll(here, ny - 1, 0))
        beside = beside + (down + up)
        left = jnp.broadcast_to(pltpu.roll(zl[...], 128 - x, 1)[:, 0:1], (ny, nz))
        right = jnp.broadcast_to(pltpu.roll(zh[...], 127 - x, 1)[:, 127:128], (ny, nz))
        left = jnp.where(zlane == 0, left, pltpu.roll(here, 1, 1))
        right = jnp.where(zlane == nz - 1, right, pltpu.roll(here, nz - 1, 1))
        beside = beside + (left + right)
        new = 0.2 * here + w_ref[x] * (rhs_ref[x] + beside)
        new_ref[x] = new
        if last:
            return totals
        put_faces(x, new, lanes, faces[2], faces[3])
        low = packed(x, new[:, 0:1], totals[0], lanes)
        high = packed(x, new[:, nz - 1 : nz], totals[1], lanes)
        return low, high

    def body(i, totals):
        for j in range(UNROLL):
            x = 1 + i * UNROLL + j
            totals = update(x, u_ref[x - 1], u_ref[x], u_ref[x + 1], totals)
        return totals

    zero = jnp.zeros((ny, 128), jnp.float32)
    totals = update(0, xl[...], u_ref[0], u_ref[1], (zero, zero))
    steps = (nx - 2) // UNROLL
    totals = lax.fori_loop(0, steps, body, totals)
    for x in range(1 + steps * UNROLL, nx - 1):
        totals = update(x, u_ref[x - 1], u_ref[x], u_ref[x + 1], totals)
    totals = update(nx - 1, u_ref[nx - 2], u_ref[nx - 1], xh[...], totals)
    if not last:
        faces[0][...] = new_ref[0]
        faces[1][...] = new_ref[nx - 1]
        faces[4][...], faces[5][...] = totals


def exchange(faces):
    halos = []
    for axis, low, high in (("gx", 0, 1), ("gy", 2, 3), ("gz", 4, 5)):
        peers = lax.axis_size(axis)
        up = [(i, (i + 1) % peers) for i in range(peers)]
        halos.append(lax.ppermute(faces[high], axis, up))
        halos.append(lax.ppermute(faces[low], axis, [(b, a) for a, b in up]))
    return halos


def shards(initial, right_side, shift_field):
    nx, ny, nz = initial.shape
    face = [(ny, nz)] * 2 + [(nx, nz)] * 2 + [(ny, 128)] * 2
    faces = call(pack_kernel, face, (initial,), nx * ny * nz)
    halos = exchange(faces)
    (w,) = call(weight_kernel, [initial.shape], (shift_field,), 8 * nx * ny * nz)
    relaxed = initial
    for sweep in range(SWEEPS):
        last = sweep == SWEEPS - 1
        outs = [initial.shape] + ([] if last else face)
        relaxed, *faces = call(
            functools.partial(sweep_kernel, last),
            outs,
            (relaxed, right_side, w, *halos),
            14 * nx * ny * nz,
        )
        if not last:
            halos = exchange(faces)
    return relaxed


def solution(mesh):
    spec = P("gx", "gy", "gz")
    return jax.shard_map(shards, mesh=mesh, in_specs=(spec,) * 3, out_specs=spec, check_vma=False)
```

```python
import functools

import jax
import jax.numpy as jnp
from jax import lax
from jax.experimental import pallas as pl
from jax.experimental.pallas import tpu as pltpu
from jax.sharding import PartitionSpec as P

SWEEPS = 4
WIDE = 4
WEIGHT = 0.8
VMEM = pl.BlockSpec(memory_space=pltpu.VMEM)
HBM = pl.BlockSpec(memory_space=pl.ANY)
F32 = jnp.float32


def call(kernel, outs, operands, flops, scratch=(), in_hbm=False, limit=24):
    return pl.pallas_call(
        kernel,
        out_shape=[jax.ShapeDtypeStruct(s, F32) for s in outs],
        in_specs=[VMEM] * len(operands),
        out_specs=[HBM if in_hbm else VMEM] * len(outs),
        scratch_shapes=scratch,
        compiler_params=pltpu.CompilerParams(vmem_limit_bytes=limit * 2**20),
        cost_estimate=pl.CostEstimate(flops=flops, bytes_accessed=2**20, transcendentals=0),
    )(*operands)


def odd(axis):
    return lax.rem(lax.axis_index(axis), 2)


def swap(sent, axis):
    n = lax.axis_size(axis)
    near = [(i, i ^ 1) for i in range(n)]
    far = [(i, (i + (1 if i % 2 else -1)) % n) for i in range(n)]
    return lax.ppermute(sent[0], axis, near), lax.ppermute(sent[1], axis, far)


def iota(shape, dim):
    return lax.broadcasted_iota(jnp.int32, shape, dim)


def fold(first, second, low):
    row = iota(first.shape, 0)
    keep = jnp.where(low, row, 7 - row) < 4
    return jnp.where(keep, first, pltpu.roll(second, 4, 0))


def unfold(above, below):
    head = iota(above.shape, 0) < 4
    return jnp.where(head, above, below), pltpu.roll(jnp.where(head, below, above), 4, 0)


def pack_y(u, r, s, near, far):
    ny = u.shape[1]
    is_odd = odd("gy") == 1
    for face, low in ((near, is_odd), (far, jnp.logical_not(is_odd))):
        start = pl.multiple_of(jnp.where(low, 0, ny - 8), 8)
        for a, ref in enumerate((u, r, s)):

            def body(i, c, ref=ref, face=face, low=low, start=start, a=a):
                rows = pl.ds(start, 8)
                face[a, i] = fold(ref[2 * i, rows, :], ref[2 * i + 1, rows, :], low)
                return c

            lax.fori_loop(0, u.shape[0] // 2, body, 0, unroll=8)


def pack_x(u, r, s, near, far):
    nx = u.shape[0]
    is_odd = odd("gx") == 1
    for face, low in ((near, is_odd), (far, jnp.logical_not(is_odd))):
        put = 0
        for ref, layers in ((u, WIDE), (r, WIDE - 1), (s, WIDE - 1)):
            start = jnp.where(low, 0, nx - layers)
            for k in range(layers):
                face[put] = ref[start + k]
                put += 1


def pack_z(u, r, s, near, far):
    nx, ny, nz = u.shape
    block = iota((ny, 128), 1) // 4
    half = iota((ny, 128), 1) < 64
    is_odd = odd("gz") == 1
    for a, ref in enumerate((u, r, s)):

        def body(g, c, ref=ref, a=a):
            low = jnp.zeros((ny, 128), F32)
            high = low
            for j in range(32):
                x = g * 32 + j
                both = jnp.where(half, ref[x, :, 0:128], ref[x, :, nz - 128 : nz])
                both = pltpu.roll(both, 4 * j, 1) if j else both
                low = jnp.where(block == j, both, low)
                high = jnp.where(block == (j - 1) % 32, both, high)
            near[a, g] = jnp.where(is_odd, low, high)
            far[a, g] = jnp.where(is_odd, high, low)
            return c

        lax.fori_loop(0, nx // 32, body, 0)


def pack_yz(za, zb, near, far):
    ny = za.shape[2]
    is_odd = odd("gy") == 1
    for face, low in ((near, is_odd), (far, jnp.logical_not(is_odd))):
        rows = pl.ds(pl.multiple_of(jnp.where(low, 0, ny - 8), 8), 8)
        for a in range(3):
            for g in range(za.shape[1]):
                face[a, g] = fold(za[a, g, rows, :], zb[a, g, rows, :], low)


def weight(shift):
    return WEIGHT / (6.0 + shift)


def weigh(s, w):
    def body(i, c):
        w[i] = weight(s[i])
        return c

    lax.fori_loop(0, s.shape[0], body, 0, unroll=2)


def spread_z(high, low, j):
    tile = jnp.where(iota(high.shape, 1) // 4 == j, high, low)
    return pltpu.roll(tile, 128 - 4 * j, 1) if j else tile


def unpack_z(za, zb, tu, tr, tw):
    is_odd = odd("gz") == 1
    for a, out in enumerate((tu, tr, tw)):

        def body(g, c, a=a, out=out):
            one, two = za[a, g], zb[a, g]
            high, low = jnp.where(is_odd, two, one), jnp.where(is_odd, one, two)
            for j in range(32):
                tile = spread_z(high, low, j)
                out[g * 32 + j] = weight(tile) if a == 2 else tile
            return c

        lax.fori_loop(0, za.shape[1], body, 0)


def unpack_y(u_y, u_f, b_y, b_f, yu, yr, yw, tu, tr, tw):
    is_odd = odd("gy") == 1
    z_odd = odd("gz") == 1
    for a, out in enumerate((yu, yr, yw)):

        def body(i, c, a=a, out=out):
            one, two = u_y[a, i], u_f[a, i]
            above, below = jnp.where(is_odd, two, one), jnp.where(is_odd, one, two)
            first, second = unfold(above, below)
            out[2 * i] = weight(first) if a == 2 else first
            out[2 * i + 1] = weight(second) if a == 2 else second
            return c

        lax.fori_loop(0, u_y.shape[1], body, 0, unroll=4)
    for a, out in enumerate((tu, tr, tw)):
        for g in range(b_y.shape[1]):
            one, two = b_y[a, g], b_f[a, g]
            above, below = jnp.where(is_odd, two, one), jnp.where(is_odd, one, two)
            near, far = unfold(above, below)
            high, low = jnp.where(z_odd, far, near), jnp.where(z_odd, near, far)
            for j in range(32):
                tile = spread_z(high, low, j)
                out[g * 32 + j] = weight(tile) if a == 2 else tile


LAYERS = [(a, k) for a, n in enumerate((WIDE, WIDE - 1, WIDE - 1)) for k in range(n)]


def pack_edges(yu, yr, yw, tu, tr, tw, eu, er, ew, near, far):
    nx = yu.shape[0]
    is_odd = odd("gx") == 1
    lane = iota((8, 128), 1) // 8
    for face, low in ((near, is_odd), (far, jnp.logical_not(is_odd))):
        total = [jnp.zeros((8, 128), F32)] * 5
        for q, (a, k) in enumerate(LAYERS):
            layers = WIDE if a == 0 else WIDE - 1
            x = jnp.where(low, k, nx - layers + k)
            face[q] = (yu, yr, yw)[a][x]
            for t in range(5):
                tile = (tu, tr, tw)[a][x, 8 * t : 8 * t + 8, :] if t < 4 else (eu, er, ew)[a][x]
                total[t] = jnp.where(lane == q, pltpu.roll(tile, 8 * q + 4, 1), total[t])
        for t in range(6):
            face[len(LAYERS) + t // 2, :, 128 * (t % 2) : 128 * (t % 2) + 128] = total[min(t, 4)]


def stencil(below, here, above, r, w):
    n, m = here.shape
    beside = below + above
    beside = beside + (pltpu.roll(here, 1, 0) + pltpu.roll(here, n - 1, 0))
    beside = beside + (pltpu.roll(here, 1, 1) + pltpu.roll(here, m - 1, 1))
    return 0.2 * here + w * (r + beside)


def whole(x, main, y, t, e):
    left = jnp.concatenate([main[x], y[x]], 0)
    return jnp.concatenate([left, jnp.concatenate([t[x], e[x]], 0)], 1)


def centre(*refs):
    u0, r0, w0 = refs[0:4], refs[4:8], refs[8:12]
    out, ends = refs[12], refs[13:16]
    steps = refs[16:19]
    nx, ny, nz = u0[0].shape

    def plane(k, x):
        return whole(x, *u0) if k == 0 else steps[k - 1][x]

    for k in range(SWEEPS):
        lo, hi = k + 1, nx - 1 - k

        def one(x, k=k):
            r, w = whole(x, *r0), whole(x, *w0)
            new = stencil(plane(k, x - 1), plane(k, x), plane(k, x + 1), r, w)
            if k == SWEEPS - 1:
                out[x] = new[:ny, :nz]
            else:
                steps[k][x] = new

        def body(i, c, one=one, lo=lo):
            for j in range(2):
                one(lo + 2 * i + j)
            return c

        lax.fori_loop(0, (hi - lo) // 2, body, 0)
        if k < SWEEPS - 1:
            for j, x in enumerate((lo, lo + 1, hi - 2, hi - 1)):
                ends[k][j] = steps[k][x]


def tail(*refs):
    u0, r0, w0 = refs[0:4], refs[4:8], refs[8:12]
    body, ends = refs[12], refs[13:16]
    x_near, x_far, c_near, c_far = refs[16:20]
    out = refs[20]
    halo, last, sem = refs[21:24]
    steps = refs[24:27]
    nx, ny, nz = u0[0].shape
    wait = []
    copy = pltpu.make_async_copy(body.at[WIDE : nx - WIDE], out.at[WIDE : nx - WIDE], sem.at[0])
    copy.start()
    wait.append(copy)
    is_odd = odd("gx") == 1
    n = len(LAYERS)
    for side in (0, 1):
        flip = is_odd if side == 0 else jnp.logical_not(is_odd)
        for q, (a, k) in enumerate(LAYERS):
            main = jnp.where(flip, x_far[q], x_near[q])
            rows = jnp.where(flip, c_far[q], c_near[q])
            put = lambda v: weight(v) if a == 2 else v
            halo[side, q, :ny, :nz] = put(main)
            halo[side, q, ny:, :nz] = rows
            for t in range(5):
                at = (len(LAYERS) + t // 2, slice(None), slice(128 * (t % 2), 128 * (t % 2) + 128))
                tile = jnp.where(flip, c_far[at], c_near[at])
                halo[side, q, 8 * t : 8 * t + 8, nz:] = pltpu.roll(tile, 124 - 8 * q, 1)

    def start(a, x):
        layers = WIDE if a == 0 else WIDE - 1
        base = (0, WIDE, 2 * WIDE - 1)[a]
        if x >= nx:
            return halo[0, base + x - nx]
        if x < 0:
            return halo[1, base + layers + x]
        return whole(x, *(u0, r0, w0)[a])

    for side in (0, 1):

        def value(k, x):
            if k == 0:
                return start(0, x)
            lo, hi = k, nx - 1 - k
            for j, e in enumerate((lo, lo + 1, hi - 1, hi)):
                if x == e:
                    return ends[k - 1][j]
            return steps[k - 1][side, x - span(k)[0]]

        def span(k):
            if side == 0:
                return nx - k, nx + SWEEPS - k
            return k - SWEEPS, k

        for k in range(1, SWEEPS + 1):
            a, b = span(k)
            for x in range(a, b):
                new = stencil(value(k - 1, x - 1), value(k - 1, x), value(k - 1, x + 1), start(1, x), start(2, x))
                if k == SWEEPS:
                    last[side, x - a] = new[:ny, :nz]
                else:
                    steps[k - 1][side, x - a] = new
        a, b = span(SWEEPS)
        copy = pltpu.make_async_copy(last.at[side], out.at[a:b], sem.at[1 + side])
        copy.start()
        wait.append(copy)
    for copy in wait:
        copy.wait()


def shards(u, r, s):
    nx, ny, nz = u.shape
    cells = nx * ny * nz
    raw = (u, r, s)
    y = swap(call(pack_y, [(3, nx // 2, 8, nz)] * 2, raw, cells // 4), "gy")
    z_sent = call(pack_z, [(3, nx // 32, ny, 128)] * 2, raw, cells)
    z = swap(z_sent, "gz")
    x = swap(call(pack_x, [(len(LAYERS), ny, nz)] * 2, raw, cells // 8), "gx")
    b = swap(call(pack_yz, [(3, nx // 32, 8, 128)] * 2, z, cells // 64), "gy")
    (w,) = call(weigh, [u.shape], (s,), 8 * cells)
    t = call(unpack_z, [(nx, ny, 128)] * 3, z, 4 * cells)
    rows = call(unpack_y, [(nx, 8, nz)] * 3 + [(nx, 8, 128)] * 3, (*y, *b), cells)
    yy, e = rows[:3], rows[3:]
    c = swap(call(pack_edges, [(len(LAYERS) + 3, 8, nz)] * 2, (*yy, *t, *e), cells // 8), "gx")
    parts = [v for a, m in enumerate((u, r, w)) for v in (m, yy[a], t[a], e[a])]
    block = (ny + 2 * WIDE, nz + 128)
    scratch = [pltpu.VMEM((nx,) + block, F32)] * 3
    body, *ends = call(centre, [u.shape] + [(4,) + block] * 3, parts, 60 * cells, scratch)
    scratch = [
        pltpu.VMEM((2, len(LAYERS)) + block, F32),
        pltpu.VMEM((2, WIDE, ny, nz), F32),
        pltpu.SemaphoreType.DMA((3,)),
    ] + [pltpu.VMEM((2, SWEEPS) + block, F32)] * 3
    (out,) = call(tail, [u.shape], (*parts, body, *ends, *x, *c), 8 * cells, scratch, in_hbm=True)
    return out


def solution(mesh):
    spec = P("gx", "gy", "gz")
    return jax.shard_map(shards, mesh=mesh, in_specs=(spec,) * 3, out_specs=spec, check_vma=False)
```

```python
import jax
import jax.numpy as jnp
from jax import lax
from jax.experimental import pallas as pl
from jax.experimental.pallas import tpu as pltpu
from jax.sharding import PartitionSpec as P


SWEEPS = 4
WIDE = 4
WEIGHT = 0.8
VMEM = pl.BlockSpec(memory_space=pltpu.VMEM)
HBM = pl.BlockSpec(memory_space=pltpu.HBM)
F32 = jnp.float32


def call(kernel, outs, operands, flops, scratch=(), limit=4, from_hbm=False, to_hbm=False):
    return pl.pallas_call(
        kernel,
        out_shape=[jax.ShapeDtypeStruct(s, F32) for s in outs],
        in_specs=[HBM if from_hbm else VMEM] * len(operands),
        out_specs=[HBM if to_hbm else VMEM] * len(outs),
        scratch_shapes=scratch,
        compiler_params=pltpu.CompilerParams(vmem_limit_bytes=limit * 2**20),
        cost_estimate=pl.CostEstimate(flops=flops, bytes_accessed=2**20, transcendentals=0),
    )(*operands)


def odd(axis):
    return lax.rem(lax.axis_index(axis), 2)


def swap(sent, axis):
    n = lax.axis_size(axis)
    near = [(i, i ^ 1) for i in range(n)]
    far = [(i, (i + (1 if i % 2 else -1)) % n) for i in range(n)]
    return lax.ppermute(sent[0], axis, near), lax.ppermute(sent[1], axis, far)


def iota(shape, dim):
    return lax.broadcasted_iota(jnp.int32, shape, dim)


def fold(first, second, low):
    row = iota(first.shape, 0)
    keep = jnp.where(low, row, 7 - row) < 4
    return jnp.where(keep, first, pltpu.roll(second, 4, 0))


def unfold(above, below):
    head = iota(above.shape, 0) < 4
    return jnp.where(head, above, below), pltpu.roll(jnp.where(head, below, above), 4, 0)


def pack_y(u, r, s, near, far, ends, sem):
    ny = u.shape[1]
    is_odd = odd("gy") == 1
    copies = []
    for a, ref in enumerate((u, r, s)):
        for e, row in enumerate((0, ny - 8)):
            copy = pltpu.make_async_copy(ref.at[:, row : row + 8, :], ends.at[a, e], sem.at[a, e])
            copy.start()
            copies.append(copy)
    for a in range(3):
        copies[2 * a].wait()
        copies[2 * a + 1].wait()
        for face, low in ((near, is_odd), (far, jnp.logical_not(is_odd))):
            end = jnp.where(low, 0, 1)

            def body(i, c, face=face, low=low, end=end, a=a):
                face[a, i] = fold(ends[a, end, 2 * i], ends[a, end, 2 * i + 1], low)
                return c

            lax.fori_loop(0, u.shape[0] // 2, body, 0, unroll=8)


def pack_x(u, r, s, near, far):
    nx = u.shape[0]
    is_odd = odd("gx") == 1
    for face, low in ((near, is_odd), (far, jnp.logical_not(is_odd))):
        put = 0
        for ref, layers in ((u, WIDE), (r, WIDE - 1), (s, WIDE - 1)):
            start = jnp.where(low, 0, nx - layers)
            for k in range(layers):
                face[put] = ref[start + k]
                put += 1


def pack_z(u, r, s, near, far):
    nx, ny, nz = u.shape
    block = iota((ny, 128), 1) // 4
    half = iota((ny, 128), 1) < 64
    is_odd = odd("gz") == 1
    for a, ref in enumerate((u, r, s)):

        def body(g, c, ref=ref, a=a):
            low = jnp.zeros((ny, 128), F32)
            high = low
            for j in range(32):
                x = g * 32 + j
                both = jnp.where(half, ref[x, :, 0:128], ref[x, :, nz - 128 : nz])
                both = pltpu.roll(both, 4 * j, 1) if j else both
                low = jnp.where(block == j, both, low)
                high = jnp.where(block == (j - 1) % 32, both, high)
            near[a, g] = jnp.where(is_odd, low, high)
            far[a, g] = jnp.where(is_odd, high, low)
            return c

        lax.fori_loop(0, nx // 32, body, 0)


def pack_yz(za, zb, near, far):
    ny = za.shape[2]
    is_odd = odd("gy") == 1
    for face, low in ((near, is_odd), (far, jnp.logical_not(is_odd))):
        rows = pl.ds(pl.multiple_of(jnp.where(low, 0, ny - 8), 8), 8)
        for a in range(3):
            for g in range(za.shape[1]):
                face[a, g] = fold(za[a, g, rows, :], zb[a, g, rows, :], low)


def weight(shift):
    return WEIGHT / (6.0 + shift)


def spread_z(high, low, j):
    tile = jnp.where(iota(high.shape, 1) // 4 == j, high, low)
    return pltpu.roll(tile, 128 - 4 * j, 1) if j else tile


def unpack_z(za, zb, s, tu, tr, tw, w):
    is_odd = odd("gz") == 1

    def weigh(i, c):
        w[i] = weight(s[i])
        return c

    lax.fori_loop(0, s.shape[0], weigh, 0, unroll=2)
    for a, out in enumerate((tu, tr, tw)):

        def body(g, c, a=a, out=out):
            one, two = za[a, g], zb[a, g]
            high, low = jnp.where(is_odd, two, one), jnp.where(is_odd, one, two)
            for j in range(32):
                tile = spread_z(high, low, j)
                out[g * 32 + j] = weight(tile) if a == 2 else tile
            return c

        lax.fori_loop(0, za.shape[1], body, 0)


def unpack_y(u_y, u_f, b_y, b_f, yu, yr, yw, tu, tr, tw):
    is_odd = odd("gy") == 1
    z_odd = odd("gz") == 1
    for a, out in enumerate((yu, yr, yw)):

        def body(i, c, a=a, out=out):
            one, two = u_y[a, i], u_f[a, i]
            above, below = jnp.where(is_odd, two, one), jnp.where(is_odd, one, two)
            first, second = unfold(above, below)
            out[2 * i] = weight(first) if a == 2 else first
            out[2 * i + 1] = weight(second) if a == 2 else second
            return c

        lax.fori_loop(0, u_y.shape[1], body, 0, unroll=4)
    for a, out in enumerate((tu, tr, tw)):
        for g in range(b_y.shape[1]):
            one, two = b_y[a, g], b_f[a, g]
            above, below = jnp.where(is_odd, two, one), jnp.where(is_odd, one, two)
            near, far = unfold(above, below)
            high, low = jnp.where(z_odd, far, near), jnp.where(z_odd, near, far)
            for j in range(32):
                tile = spread_z(high, low, j)
                out[g * 32 + j] = weight(tile) if a == 2 else tile


LAYERS = [(a, k) for a, n in enumerate((WIDE, WIDE - 1, WIDE - 1)) for k in range(n)]


def pack_edges(yu, yr, yw, tu, tr, tw, eu, er, ew, near, far):
    nx = yu.shape[0]
    is_odd = odd("gx") == 1
    lane = iota((8, 128), 1) // 8
    for face, low in ((near, is_odd), (far, jnp.logical_not(is_odd))):
        total = [jnp.zeros((8, 128), F32)] * 5
        for q, (a, k) in enumerate(LAYERS):
            layers = WIDE if a == 0 else WIDE - 1
            x = jnp.where(low, k, nx - layers + k)
            face[q] = (yu, yr, yw)[a][x]
            for t in range(5):
                tile = (tu, tr, tw)[a][x, 8 * t : 8 * t + 8, :] if t < 4 else (eu, er, ew)[a][x]
                total[t] = jnp.where(lane == q, pltpu.roll(tile, 8 * q + 4, 1), total[t])
        for t in range(6):
            face[len(LAYERS) + t // 2, :, 128 * (t % 2) : 128 * (t % 2) + 128] = total[min(t, 4)]


def stencil(below, here, above, r, w):
    n, m = here.shape
    beside = below + above
    beside = beside + (pltpu.roll(here, 1, 0) + pltpu.roll(here, n - 1, 0))
    beside = beside + (pltpu.roll(here, 1, 1) + pltpu.roll(here, m - 1, 1))
    return 0.2 * here + w * (r + beside)


def whole(x, main, y, t, e):
    left = jnp.concatenate([main[x], y[x]], 0)
    return jnp.concatenate([left, jnp.concatenate([t[x], e[x]], 0)], 1)


PLANES = 2


def centre(*refs):
    u0, r0, w0 = refs[0:4], refs[4:8], refs[8:12]
    out, ends = refs[12], refs[13:16]
    steps = refs[16:19]
    nx, ny, nz = u0[0].shape

    def plane(k, x):
        return whole(x, *u0) if k == 0 else steps[k - 1][x]

    def one(k, x):
        r, w = whole(x, *r0), whole(x, *w0)
        new = stencil(plane(k, x - 1), plane(k, x), plane(k, x + 1), r, w)
        if k == SWEEPS - 1:
            out[x] = new[:ny, :nz]
        else:
            steps[k][x] = new

    def planes(i):
        return [(k, 1 + PLANES * i - k * (PLANES + 1) + j) for k in range(SWEEPS) for j in range(PLANES)]

    def valid(k, x):
        return k + 1 <= x <= nx - 2 - k

    count = -(-(nx - 1 + (SWEEPS - 1) * (PLANES + 1)) // PLANES)
    full = [i for i in range(count) if all(valid(*p) for p in planes(i))]

    def peeled(i):
        for p in planes(i):
            if valid(*p):
                one(*p)

    for i in range(full[0]):
        peeled(i)

    def body(i, c):
        for p in planes(i):
            one(*p)
        return c

    lax.fori_loop(full[0], full[-1] + 1, body, 0)
    for i in range(full[-1] + 1, count):
        peeled(i)
    for k in range(SWEEPS - 1):
        lo, hi = k + 1, nx - 1 - k
        for j, x in enumerate((lo, lo + 1, hi - 2, hi - 1)):
            ends[k][j] = steps[k][x]


def tail(*refs):
    u0, r0, w0 = refs[0:4], refs[4:8], refs[8:12]
    body, ends = refs[12], refs[13:16]
    x_near, x_far, c_near, c_far = refs[16:20]
    out = refs[20]
    halo, last, sem = refs[21:24]
    steps = refs[24:27]
    nx, ny, nz = u0[0].shape
    wait = []
    copy = pltpu.make_async_copy(body.at[WIDE : nx - WIDE], out.at[WIDE : nx - WIDE], sem.at[0])
    copy.start()
    wait.append(copy)
    is_odd = odd("gx") == 1
    for side in (0, 1):
        flip = is_odd if side == 0 else jnp.logical_not(is_odd)
        for q, (a, k) in enumerate(LAYERS):
            main = jnp.where(flip, x_far[q], x_near[q])
            rows = jnp.where(flip, c_far[q], c_near[q])
            put = lambda v: weight(v) if a == 2 else v
            halo[side, q, :ny, :nz] = put(main)
            halo[side, q, ny:, :nz] = rows
            for t in range(5):
                at = (len(LAYERS) + t // 2, slice(None), slice(128 * (t % 2), 128 * (t % 2) + 128))
                tile = jnp.where(flip, c_far[at], c_near[at])
                halo[side, q, 8 * t : 8 * t + 8, nz:] = pltpu.roll(tile, 124 - 8 * q, 1)

    def start(a, x):
        layers = WIDE if a == 0 else WIDE - 1
        base = (0, WIDE, 2 * WIDE - 1)[a]
        if x >= nx:
            return halo[0, base + x - nx]
        if x < 0:
            return halo[1, base + layers + x]
        return whole(x, *(u0, r0, w0)[a])

    for side in (0, 1):

        def value(k, x):
            if k == 0:
                return start(0, x)
            lo, hi = k, nx - 1 - k
            for j, e in enumerate((lo, lo + 1, hi - 1, hi)):
                if x == e:
                    return ends[k - 1][j]
            return steps[k - 1][side, x - span(k)[0]]

        def span(k):
            if side == 0:
                return nx - k, nx + SWEEPS - k
            return k - SWEEPS, k

        for k in range(1, SWEEPS + 1):
            a, b = span(k)
            for x in range(a, b):
                new = stencil(value(k - 1, x - 1), value(k - 1, x), value(k - 1, x + 1), start(1, x), start(2, x))
                if k == SWEEPS:
                    last[side, x - a] = new[:ny, :nz]
                else:
                    steps[k - 1][side, x - a] = new
        a, b = span(SWEEPS)
        copy = pltpu.make_async_copy(last.at[side], out.at[a:b], sem.at[1 + side])
        copy.start()
        wait.append(copy)
    for copy in wait:
        copy.wait()


def shards(u, r, s):
    nx, ny, nz = u.shape
    cells = nx * ny * nz
    raw = (u, r, s)
    scratch = [pltpu.VMEM((3, 2, nx, 8, nz), F32), pltpu.SemaphoreType.DMA((3, 2))]
    fixed = [pltpu.with_memory_space_constraint(v, pltpu.HBM) for v in raw]
    sent = call(pack_y, [(3, nx // 2, 8, nz)] * 2, fixed, cells // 4, scratch, 8, from_hbm=True)
    y = swap(sent, "gy")
    sent = call(pack_z, [(3, nx // 32, ny, 128)] * 2, raw, cells)
    z = swap(sent, "gz")
    sent = call(pack_x, [(len(LAYERS), ny, nz)] * 2, raw, cells // 8)
    x = swap(sent, "gx")
    sent = call(pack_yz, [(3, nx // 32, 8, 128)] * 2, z, cells // 64)
    b = swap(sent, "gy")
    *t, w = call(unpack_z, [(nx, ny, 128)] * 3 + [u.shape], (*z, s), 8 * cells)
    rows = call(unpack_y, [(nx, 8, nz)] * 3 + [(nx, 8, 128)] * 3, (*y, *b), cells)
    yy, e = rows[:3], rows[3:]
    sent = call(pack_edges, [(len(LAYERS) + 3, 8, nz)] * 2, (*yy, *t, *e), cells // 8)
    c = swap(sent, "gx")
    parts = [v for a, m in enumerate((u, r, w)) for v in (m, yy[a], t[a], e[a])]
    block = (ny + 2 * WIDE, nz + 128)
    scratch = [pltpu.VMEM((nx,) + block, F32)] * 3
    body, *ends = call(centre, [u.shape] + [(4,) + block] * 3, parts, 60 * cells, scratch, 16)
    scratch = [
        pltpu.VMEM((2, len(LAYERS)) + block, F32),
        pltpu.VMEM((2, WIDE, ny, nz), F32),
        pltpu.SemaphoreType.DMA((3,)),
    ] + [pltpu.VMEM((2, SWEEPS) + block, F32)] * 3
    (out,) = call(tail, [u.shape], (*parts, body, *ends, *x, *c), 8 * cells, scratch, 8, to_hbm=True)
    return out


def solution(mesh):
    spec = P("gx", "gy", "gz")
    return jax.shard_map(shards, mesh=mesh, in_specs=(spec,) * 3, out_specs=spec, check_vma=False)
```

```python
import jax
import jax.numpy as jnp
from jax import lax
from jax.experimental import pallas as pl
from jax.experimental.pallas import tpu as pltpu
from jax.sharding import PartitionSpec as P


SWEEPS = 4
WIDE = 4
WEIGHT = 0.8
VMEM = pl.BlockSpec(memory_space=pltpu.VMEM)
HBM = pl.BlockSpec(memory_space=pltpu.HBM)
F32 = jnp.float32
LAYERS = [(a, k) for a, n in enumerate((WIDE, WIDE - 1, WIDE - 1)) for k in range(n)]


def call(kernel, outs, operands, flops, scratch=(), limit=4, hbm_in=(), hbm_out=(), aliases={}):
    return pl.pallas_call(
        kernel,
        out_shape=[jax.ShapeDtypeStruct(s, F32) for s in outs],
        in_specs=[HBM if i in hbm_in else VMEM for i in range(len(operands))],
        out_specs=[HBM if i in hbm_out else VMEM for i in range(len(outs))],
        scratch_shapes=scratch,
        input_output_aliases=aliases,
        compiler_params=pltpu.CompilerParams(vmem_limit_bytes=limit * 2**20),
        cost_estimate=pl.CostEstimate(flops=flops, bytes_accessed=2**20, transcendentals=0),
    )(*operands)


def odd(axis):
    return lax.rem(lax.axis_index(axis), 2)


def swap(sent, axis):
    n = lax.axis_size(axis)
    near = [(i, i ^ 1) for i in range(n)]
    far = [(i, (i + (1 if i % 2 else -1)) % n) for i in range(n)]
    return lax.ppermute(sent[0], axis, near), lax.ppermute(sent[1], axis, far)


def iota(shape, dim):
    return lax.broadcasted_iota(jnp.int32, shape, dim)


def fold(first, second, low):
    row = iota(first.shape, 0)
    keep = jnp.where(low, row, 7 - row) < 4
    return jnp.where(keep, first, pltpu.roll(second, 4, 0))


def unfold(above, below):
    head = iota(above.shape, 0) < 4
    return jnp.where(head, above, below), pltpu.roll(jnp.where(head, below, above), 4, 0)


def pack_y(u, r, s, near, far, ends, sem):
    ny = u.shape[1]
    is_odd = odd("gy") == 1
    copies = []
    for a, ref in enumerate((u, r, s)):
        for e, row in enumerate((0, ny - 8)):
            copy = pltpu.make_async_copy(ref.at[:, row : row + 8, :], ends.at[a, e], sem.at[a, e])
            copy.start()
            copies.append(copy)
    for a in range(3):
        copies[2 * a].wait()
        copies[2 * a + 1].wait()
        for face, low in ((near, is_odd), (far, jnp.logical_not(is_odd))):
            end = jnp.where(low, 0, 1)

            def body(i, c, face=face, low=low, end=end, a=a):
                face[a, i] = fold(ends[a, end, 2 * i], ends[a, end, 2 * i + 1], low)
                return c

            lax.fori_loop(0, u.shape[0] // 2, body, 0, unroll=8)


def pack_x(u, r, s, near, far):
    nx = u.shape[0]
    is_odd = odd("gx") == 1
    for face, low in ((near, is_odd), (far, jnp.logical_not(is_odd))):
        put = 0
        for ref, layers in ((u, WIDE), (r, WIDE - 1), (s, WIDE - 1)):
            start = jnp.where(low, 0, nx - layers)
            for k in range(layers):
                face[put] = ref[start + k]
                put += 1


def pack_z(u, r, s, near, far):
    nx, ny, nz = u.shape
    block = iota((ny, 128), 1) // 4
    half = iota((ny, 128), 1) < 64
    is_odd = odd("gz") == 1
    for a, ref in enumerate((u, r, s)):

        def body(g, c, ref=ref, a=a):
            low = jnp.zeros((ny, 128), F32)
            high = low
            for j in range(32):
                x = g * 32 + j
                both = jnp.where(half, ref[x, :, 0:128], ref[x, :, nz - 128 : nz])
                both = pltpu.roll(both, 4 * j, 1) if j else both
                low = jnp.where(block == j, both, low)
                high = jnp.where(block == (j - 1) % 32, both, high)
            near[a, g] = jnp.where(is_odd, low, high)
            far[a, g] = jnp.where(is_odd, high, low)
            return c

        lax.fori_loop(0, nx // 32, body, 0)


def pack_yz(za, zb, near, far):
    ny = za.shape[2]
    is_odd = odd("gy") == 1
    for face, low in ((near, is_odd), (far, jnp.logical_not(is_odd))):
        rows = pl.ds(pl.multiple_of(jnp.where(low, 0, ny - 8), 8), 8)
        for a in range(3):
            for g in range(za.shape[1]):
                face[a, g] = fold(za[a, g, rows, :], zb[a, g, rows, :], low)


def weight(shift):
    return WEIGHT / (6.0 + shift)


def spread_z(high, low, j):
    tile = jnp.where(iota(high.shape, 1) // 4 == j, high, low)
    return pltpu.roll(tile, 128 - 4 * j, 1) if j else tile


def weigh(s, w):
    def body(i, c):
        w[i] = weight(s[i])
        return c

    lax.fori_loop(0, s.shape[0], body, 0, unroll=2)


def unpack_z(za, zb, tu, tr, tw):
    is_odd = odd("gz") == 1
    for a, out in enumerate((tu, tr, tw)):

        def body(g, c, a=a, out=out):
            one, two = za[a, g], zb[a, g]
            high, low = jnp.where(is_odd, two, one), jnp.where(is_odd, one, two)
            for j in range(32):
                tile = spread_z(high, low, j)
                out[g * 32 + j] = weight(tile) if a == 2 else tile
            return c

        lax.fori_loop(0, za.shape[1], body, 0)


def unpack_y(near, far, yu, yr, yw):
    is_odd = odd("gy") == 1
    for a, out in enumerate((yu, yr, yw)):

        def body(i, c, a=a, out=out):
            one, two = near[a, i], far[a, i]
            above, below = jnp.where(is_odd, two, one), jnp.where(is_odd, one, two)
            first, second = unfold(above, below)
            out[2 * i] = weight(first) if a == 2 else first
            out[2 * i + 1] = weight(second) if a == 2 else second
            return c

        lax.fori_loop(0, near.shape[1], body, 0, unroll=4)


def pack_edges(b_near, b_far, yu, yr, yw, tu, tr, tw, eu, er, ew, near, far):
    y_odd, z_odd, x_odd = odd("gy") == 1, odd("gz") == 1, odd("gx") == 1
    for a, out in enumerate((eu, er, ew)):
        for g in range(b_near.shape[1]):
            one, two = b_near[a, g], b_far[a, g]
            above, below = jnp.where(y_odd, two, one), jnp.where(y_odd, one, two)
            first, second = unfold(above, below)
            high, low = jnp.where(z_odd, second, first), jnp.where(z_odd, first, second)
            for j in range(32):
                tile = spread_z(high, low, j)
                out[g * 32 + j] = weight(tile) if a == 2 else tile
    nx = yu.shape[0]
    lane = iota((8, 128), 1) // 8
    for face, low in ((near, x_odd), (far, jnp.logical_not(x_odd))):
        total = [jnp.zeros((8, 128), F32)] * 5
        for q, (a, k) in enumerate(LAYERS):
            layers = WIDE if a == 0 else WIDE - 1
            x = jnp.where(low, k, nx - layers + k)
            face[q] = (yu, yr, yw)[a][x]
            for t in range(5):
                tile = (tu, tr, tw)[a][x, 8 * t : 8 * t + 8, :] if t < 4 else (eu, er, ew)[a][x]
                total[t] = jnp.where(lane == q, pltpu.roll(tile, 8 * q + 4, 1), total[t])
        for t in range(6):
            face[len(LAYERS) + t // 2, :, 128 * (t % 2) : 128 * (t % 2) + 128] = total[min(t, 4)]


def stencil(below, here, above, r, w):
    n, m = here.shape
    beside = below + above
    beside = beside + (pltpu.roll(here, 1, 0) + pltpu.roll(here, n - 1, 0))
    beside = beside + (pltpu.roll(here, 1, 1) + pltpu.roll(here, m - 1, 1))
    return 0.2 * here + w * (r + beside)


def whole(x, main, y, t, e):
    left = jnp.concatenate([main[x], y[x]], 0)
    return jnp.concatenate([left, jnp.concatenate([t[x], e[x]], 0)], 1)


PLANES = 2


def planes(i):
    return [(k, 1 + PLANES * i - k * (PLANES + 1) + j) for k in range(SWEEPS) for j in range(PLANES)]


def steps_of(nx):
    def valid(k, x):
        return k + 1 <= x <= nx - 2 - k

    count = -(-(nx - 1 + (SWEEPS - 1) * (PLANES + 1)) // PLANES)
    done = [[p for p in planes(i) if valid(*p)] for i in range(count)]
    full = [i for i in range(count) if len(done[i]) == SWEEPS * PLANES]
    first = planes(full[0])[-PLANES][1]
    stop = planes(full[-1])[-1][1] + 1
    return done, full, first, stop


def centre(*refs):
    u0, r0, w0 = refs[0:4], refs[4:8], refs[8:12]
    out, rest, ends = refs[12], refs[13], refs[14:17]
    last, sem = refs[17:19]
    steps = refs[19:22]
    nx, ny, nz = u0[0].shape
    done, full, first, stop = steps_of(nx)

    def plane(k, x):
        return whole(x, *u0) if k == 0 else steps[k - 1][x]

    def one(k, x):
        r, w = whole(x, *r0), whole(x, *w0)
        new = stencil(plane(k, x - 1), plane(k, x), plane(k, x + 1), r, w)
        if k < SWEEPS - 1:
            steps[k][x] = new
        elif isinstance(x, int):
            rest[x - stop if x >= stop else nx - WIDE - stop + x - WIDE] = new[:ny, :nz]
        else:
            last[x] = new[:ny, :nz]

    for i in range(full[0]):
        for p in done[i]:
            one(*p)

    def body(i, c):
        for p in planes(i):
            one(*p)
        at = pl.ds(planes(i)[-PLANES][1], PLANES)
        pltpu.make_async_copy(last.at[at], out.at[at], sem).start()
        return c

    lax.fori_loop(full[0], full[-1] + 1, body, 0)
    for i in range(full[-1] + 1, len(done)):
        for p in done[i]:
            one(*p)
    for k in range(SWEEPS - 1):
        lo, hi = k + 1, nx - 1 - k
        for j, x in enumerate((lo, lo + 1, hi - 2, hi - 1)):
            ends[k][j] = steps[k][x]
    pltpu.make_async_copy(last.at[first:stop], out.at[first:stop], sem).wait()


def tail(*refs):
    u0, r0, w0 = refs[0:4], refs[4:8], refs[8:12]
    rest, ends = refs[13], refs[14:17]
    x_near, x_far, c_near, c_far = refs[17:21]
    out = refs[21]
    halo, last, sem = refs[22:25]
    steps = refs[25:28]
    nx, ny, nz = u0[0].shape
    _, _, first, stop = steps_of(nx)
    wait = []
    if first > WIDE:
        wait.append(pltpu.make_async_copy(rest.at[nx - WIDE - stop :], out.at[WIDE:first], sem.at[2]))
    wait.append(pltpu.make_async_copy(rest.at[: nx - WIDE - stop], out.at[stop : nx - WIDE], sem.at[3]))
    for copy in wait:
        copy.start()
    is_odd = odd("gx") == 1
    for side in (0, 1):
        flip = is_odd if side == 0 else jnp.logical_not(is_odd)
        for q, (a, k) in enumerate(LAYERS):
            main = jnp.where(flip, x_far[q], x_near[q])
            rows = jnp.where(flip, c_far[q], c_near[q])
            put = lambda v: weight(v) if a == 2 else v
            halo[side, q, :ny, :nz] = put(main)
            halo[side, q, ny:, :nz] = rows
            for t in range(5):
                at = (len(LAYERS) + t // 2, slice(None), slice(128 * (t % 2), 128 * (t % 2) + 128))
                tile = jnp.where(flip, c_far[at], c_near[at])
                halo[side, q, 8 * t : 8 * t + 8, nz:] = pltpu.roll(tile, 124 - 8 * q, 1)

    def start(a, x):
        layers = WIDE if a == 0 else WIDE - 1
        base = (0, WIDE, 2 * WIDE - 1)[a]
        if x >= nx:
            return halo[0, base + x - nx]
        if x < 0:
            return halo[1, base + layers + x]
        return whole(x, *(u0, r0, w0)[a])

    def span(side, k):
        return (nx - k, nx + SWEEPS - k) if side == 0 else (k - SWEEPS, k)

    def value(side, k, x):
        if k == 0:
            return start(0, x)
        for j, e in enumerate((k, k + 1, nx - 2 - k, nx - 1 - k)):
            if x == e:
                return ends[k - 1][j]
        return steps[k - 1][side, x - span(side, k)[0]]

    for k in range(1, SWEEPS + 1):
        for j in range(SWEEPS):
            for side in (0, 1):
                x = span(side, k)[0] + j
                near = [value(side, k - 1, x + d) for d in (-1, 0, 1)]
                new = stencil(*near, start(1, x), start(2, x))
                if k == SWEEPS:
                    last[side, j] = new[:ny, :nz]
                else:
                    steps[k - 1][side, j] = new
    for side in (0, 1):
        a, b = span(side, SWEEPS)
        copy = pltpu.make_async_copy(last.at[side], out.at[a:b], sem.at[side])
        copy.start()
        wait.append(copy)
    for copy in wait:
        copy.wait()


def shards(u, r, s):
    nx, ny, nz = u.shape
    cells = nx * ny * nz
    raw = (u, r, s)
    fixed = [pltpu.with_memory_space_constraint(v, pltpu.HBM) for v in raw]
    scratch = [pltpu.VMEM((3, 2, nx, 8, nz), F32), pltpu.SemaphoreType.DMA((3, 2))]
    sent = call(pack_y, [(3, nx // 2, 8, nz)] * 2, fixed, cells // 4, scratch, 8, hbm_in=range(3))
    y = swap(sent, "gy")
    sent = call(pack_z, [(3, nx // 32, ny, 128)] * 2, raw, cells)
    z = swap(sent, "gz")
    sent = call(pack_x, [(len(LAYERS), ny, nz)] * 2, raw, cells // 8)
    x = swap(sent, "gx")
    (w,) = call(weigh, [u.shape], (s,), 8 * cells)
    sent = call(pack_yz, [(3, nx // 32, 8, 128)] * 2, z, cells // 64)
    b = swap(sent, "gy")
    t = call(unpack_z, [(nx, ny, 128)] * 3, z, 8 * cells)
    yy = call(unpack_y, [(nx, 8, nz)] * 3, y, cells)
    shape = (len(LAYERS) + 3, 8, nz)
    *e, c_near, c_far = call(pack_edges, [(nx, 8, 128)] * 3 + [shape] * 2, (*b, *yy, *t), cells // 8)
    c = swap((c_near, c_far), "gx")
    parts = [v for a, m in enumerate((u, r, w)) for v in (m, yy[a], t[a], e[a])]
    block = (ny + 2 * WIDE, nz + 128)
    _, _, first, stop = steps_of(nx)
    scratch = [pltpu.VMEM(u.shape, F32), pltpu.SemaphoreType.DMA] + [pltpu.VMEM((nx,) + block, F32)] * 3
    left = (nx - WIDE - stop + first - WIDE, ny, nz)
    out, rest, *ends = call(
        centre, [u.shape, left] + [(4,) + block] * 3, parts, 60 * cells, scratch, 16, hbm_out=(0,)
    )
    scratch = [
        pltpu.VMEM((2, len(LAYERS)) + block, F32),
        pltpu.VMEM((2, WIDE, ny, nz), F32),
        pltpu.SemaphoreType.DMA((4,)),
    ] + [pltpu.VMEM((2, SWEEPS) + block, F32)] * 3
    operands = (*parts, out, rest, *ends, *x, *c)
    (out,) = call(
        tail, [u.shape], operands, 8 * cells, scratch, 8, hbm_in=(12,), hbm_out=(0,), aliases={12: 0}
    )
    return out


def solution(mesh):
    spec = P("gx", "gy", "gz")
    return jax.shard_map(shards, mesh=mesh, in_specs=(spec,) * 3, out_specs=spec, check_vma=False)
```

```python
import jax
import jax.numpy as jnp
from jax import lax
from jax.experimental import pallas as pl
from jax.experimental.pallas import tpu as pltpu
from jax.sharding import PartitionSpec as P


SWEEPS = 4
WIDE = 4
WEIGHT = 0.8
VMEM = pl.BlockSpec(memory_space=pltpu.VMEM)
HBM = pl.BlockSpec(memory_space=pltpu.HBM)
F32 = jnp.float32
LAYERS = [(a, k) for a, n in enumerate((WIDE, WIDE - 1, WIDE - 1)) for k in range(n)]


def call(kernel, outs, operands, flops, scratch=(), limit=4, hbm_in=(), hbm_out=(), aliases={}):
    return pl.pallas_call(
        kernel,
        out_shape=[jax.ShapeDtypeStruct(s, F32) for s in outs],
        in_specs=[HBM if i in hbm_in else VMEM for i in range(len(operands))],
        out_specs=[HBM if i in hbm_out else VMEM for i in range(len(outs))],
        scratch_shapes=scratch,
        input_output_aliases=aliases,
        compiler_params=pltpu.CompilerParams(vmem_limit_bytes=limit * 2**20),
        cost_estimate=pl.CostEstimate(flops=flops, bytes_accessed=2**20, transcendentals=0),
    )(*operands)


def odd(axis):
    return lax.rem(lax.axis_index(axis), 2)


def swap(sent, axis):
    n = lax.axis_size(axis)
    near = [(i, i ^ 1) for i in range(n)]
    far = [(i, (i + (1 if i % 2 else -1)) % n) for i in range(n)]
    return lax.ppermute(sent[0], axis, near), lax.ppermute(sent[1], axis, far)


def iota(shape, dim):
    return lax.broadcasted_iota(jnp.int32, shape, dim)


def fold(first, second, low):
    row = iota(first.shape, 0)
    keep = jnp.where(low, row, 7 - row) < 4
    return jnp.where(keep, first, pltpu.roll(second, 4, 0))


def unfold(above, below):
    head = iota(above.shape, 0) < 4
    return jnp.where(head, above, below), pltpu.roll(jnp.where(head, below, above), 4, 0)


def pack_y(u, r, s, near, far, ends, sem):
    ny = u.shape[1]
    is_odd = odd("gy") == 1
    copies = []
    for a, ref in enumerate((u, r, s)):
        for e, row in enumerate((0, ny - 8)):
            copy = pltpu.make_async_copy(ref.at[:, row : row + 8, :], ends.at[a, e], sem.at[a, e])
            copy.start()
            copies.append(copy)
    for a in range(3):
        copies[2 * a].wait()
        copies[2 * a + 1].wait()
        for face, low in ((near, is_odd), (far, jnp.logical_not(is_odd))):
            end = jnp.where(low, 0, 1)

            def body(i, c, face=face, low=low, end=end, a=a):
                face[a, i] = fold(ends[a, end, 2 * i], ends[a, end, 2 * i + 1], low)
                return c

            lax.fori_loop(0, u.shape[0] // 2, body, 0, unroll=8)


def pack_x(u, r, s, near, far):
    nx = u.shape[0]
    is_odd = odd("gx") == 1
    for face, low in ((near, is_odd), (far, jnp.logical_not(is_odd))):
        put = 0
        for ref, layers in ((u, WIDE), (r, WIDE - 1), (s, WIDE - 1)):
            start = jnp.where(low, 0, nx - layers)
            for k in range(layers):
                face[put] = ref[start + k]
                put += 1


def pack_z(u, r, s, near, far):
    nx, ny, nz = u.shape
    block = iota((ny, 128), 1) // 4
    half = iota((ny, 128), 1) < 64
    is_odd = odd("gz") == 1
    for a, ref in enumerate((u, r, s)):

        def body(g, c, ref=ref, a=a):
            low = jnp.zeros((ny, 128), F32)
            high = low
            for j in range(32):
                x = g * 32 + j
                both = jnp.where(half, ref[x, :, 0:128], ref[x, :, nz - 128 : nz])
                both = pltpu.roll(both, 4 * j, 1) if j else both
                low = jnp.where(block == j, both, low)
                high = jnp.where(block == (j - 1) % 32, both, high)
            near[a, g] = jnp.where(is_odd, low, high)
            far[a, g] = jnp.where(is_odd, high, low)
            return c

        lax.fori_loop(0, nx // 32, body, 0)


def pack_yz(za, zb, near, far):
    ny = za.shape[2]
    is_odd = odd("gy") == 1
    for face, low in ((near, is_odd), (far, jnp.logical_not(is_odd))):
        rows = pl.ds(pl.multiple_of(jnp.where(low, 0, ny - 8), 8), 8)
        for a in range(3):
            for g in range(za.shape[1]):
                face[a, g] = fold(za[a, g, rows, :], zb[a, g, rows, :], low)


def weight(shift):
    return WEIGHT / (6.0 + shift)


def spread_z(high, low, j):
    tile = jnp.where(iota(high.shape, 1) // 4 == j, high, low)
    return pltpu.roll(tile, 128 - 4 * j, 1) if j else tile


def weigh(s, w):
    def body(i, c):
        w[i] = weight(s[i])
        return c

    lax.fori_loop(0, s.shape[0], body, 0, unroll=2)


def unpack_z(za, zb, tu, tr, tw):
    is_odd = odd("gz") == 1
    for a, out in enumerate((tu, tr, tw)):

        def body(g, c, a=a, out=out):
            one, two = za[a, g], zb[a, g]
            high, low = jnp.where(is_odd, two, one), jnp.where(is_odd, one, two)
            for j in range(32):
                tile = spread_z(high, low, j)
                out[g * 32 + j] = weight(tile) if a == 2 else tile
            return c

        lax.fori_loop(0, za.shape[1], body, 0)


def unpack_y(near, far, yu, yr, yw):
    is_odd = odd("gy") == 1
    for a, out in enumerate((yu, yr, yw)):

        def body(i, c, a=a, out=out):
            one, two = near[a, i], far[a, i]
            above, below = jnp.where(is_odd, two, one), jnp.where(is_odd, one, two)
            first, second = unfold(above, below)
            out[2 * i] = weight(first) if a == 2 else first
            out[2 * i + 1] = weight(second) if a == 2 else second
            return c

        lax.fori_loop(0, near.shape[1], body, 0, unroll=4)


def pack_edges(b_near, b_far, yu, yr, yw, tu, tr, tw, eu, er, ew, near, far):
    y_odd, z_odd, x_odd = odd("gy") == 1, odd("gz") == 1, odd("gx") == 1
    for a, out in enumerate((eu, er, ew)):
        for g in range(b_near.shape[1]):
            one, two = b_near[a, g], b_far[a, g]
            above, below = jnp.where(y_odd, two, one), jnp.where(y_odd, one, two)
            first, second = unfold(above, below)
            high, low = jnp.where(z_odd, second, first), jnp.where(z_odd, first, second)
            for j in range(32):
                tile = spread_z(high, low, j)
                out[g * 32 + j] = weight(tile) if a == 2 else tile
    nx = yu.shape[0]
    lane = iota((8, 128), 1) // 8
    for face, low in ((near, x_odd), (far, jnp.logical_not(x_odd))):
        total = [jnp.zeros((8, 128), F32)] * 5
        for q, (a, k) in enumerate(LAYERS):
            layers = WIDE if a == 0 else WIDE - 1
            x = jnp.where(low, k, nx - layers + k)
            face[q] = (yu, yr, yw)[a][x]
            for t in range(5):
                tile = (tu, tr, tw)[a][x, 8 * t : 8 * t + 8, :] if t < 4 else (eu, er, ew)[a][x]
                total[t] = jnp.where(lane == q, pltpu.roll(tile, 8 * q + 4, 1), total[t])
        for t in range(6):
            face[len(LAYERS) + t // 2, :, 128 * (t % 2) : 128 * (t % 2) + 128] = total[min(t, 4)]


def stencil(below, here, above, r, w):
    n, m = here.shape
    beside = below + above
    beside = beside + (pltpu.roll(here, 1, 0) + pltpu.roll(here, n - 1, 0))
    beside = beside + (pltpu.roll(here, 1, 1) + pltpu.roll(here, m - 1, 1))
    return 0.2 * here + w * (r + beside)


def whole(x, main, y, t, e):
    left = jnp.concatenate([main[x], y[x]], 0)
    return jnp.concatenate([left, jnp.concatenate([t[x], e[x]], 0)], 1)


PLANES = 4


def planes(i):
    return [(k, 1 + PLANES * i - k * (PLANES + 1) + j) for k in range(SWEEPS) for j in range(PLANES)]


def steps_of(nx):
    def valid(k, x):
        return k + 1 <= x <= nx - 2 - k

    count = -(-(nx - 1 + (SWEEPS - 1) * (PLANES + 1)) // PLANES)
    done = [[p for p in planes(i) if valid(*p)] for i in range(count)]
    full = [i for i in range(count) if len(done[i]) == SWEEPS * PLANES]
    first = planes(full[0])[-PLANES][1]
    stop = planes(full[-1])[-1][1] + 1
    return done, full, first, stop


def centre(*refs):
    u0, r0, w0 = refs[0:4], refs[4:8], refs[8:12]
    out, rest, ends = refs[12], refs[13], refs[14:17]
    last, sem = refs[17:19]
    steps = refs[19:22]
    nx, ny, nz = u0[0].shape
    done, full, first, stop = steps_of(nx)

    def plane(k, x):
        return whole(x, *u0) if k == 0 else steps[k - 1][x]

    def one(k, x):
        r, w = whole(x, *r0), whole(x, *w0)
        new = stencil(plane(k, x - 1), plane(k, x), plane(k, x + 1), r, w)
        if k < SWEEPS - 2:
            steps[k][x] = new
        elif k == SWEEPS - 2:
            steps[k][x, :, :nz] = new[:, :nz]
            steps[k][x, :ny, nz:] = new[:ny, nz:]
        elif isinstance(x, int):
            rest[x - stop if x >= stop else nx - WIDE - stop + x - WIDE] = new[:ny, :nz]
        else:
            last[x] = new[:ny, :nz]

    for i in range(full[0]):
        for p in done[i]:
            one(*p)

    def body(i, c):
        for p in planes(i):
            one(*p)
        at = pl.ds(planes(i)[-PLANES][1], PLANES)
        pltpu.make_async_copy(last.at[at], out.at[at], sem).start()
        return c

    lax.fori_loop(full[0], full[-1] + 1, body, 0)
    for i in range(full[-1] + 1, len(done)):
        for p in done[i]:
            one(*p)
    for k in range(SWEEPS - 1):
        lo, hi = k + 1, nx - 1 - k
        for j, x in enumerate((lo, lo + 1, hi - 2, hi - 1)):
            ends[k][j] = steps[k][x]
    pltpu.make_async_copy(last.at[first:stop], out.at[first:stop], sem).wait()


def tail(*refs):
    u0, r0, w0 = refs[0:4], refs[4:8], refs[8:12]
    rest, ends = refs[13], refs[14:17]
    x_near, x_far, c_near, c_far = refs[17:21]
    out = refs[21]
    halo, last, sem = refs[22:25]
    steps = refs[25:28]
    nx, ny, nz = u0[0].shape
    _, _, first, stop = steps_of(nx)
    wait = []
    if first > WIDE:
        wait.append(pltpu.make_async_copy(rest.at[nx - WIDE - stop :], out.at[WIDE:first], sem.at[2]))
    wait.append(pltpu.make_async_copy(rest.at[: nx - WIDE - stop], out.at[stop : nx - WIDE], sem.at[3]))
    for copy in wait:
        copy.start()
    is_odd = odd("gx") == 1
    for side in (0, 1):
        flip = is_odd if side == 0 else jnp.logical_not(is_odd)
        for q, (a, k) in enumerate(LAYERS):
            main = jnp.where(flip, x_far[q], x_near[q])
            rows = jnp.where(flip, c_far[q], c_near[q])
            put = lambda v: weight(v) if a == 2 else v
            halo[side, q, :ny, :nz] = put(main)
            halo[side, q, ny:, :nz] = rows
            for t in range(5):
                at = (len(LAYERS) + t // 2, slice(None), slice(128 * (t % 2), 128 * (t % 2) + 128))
                tile = jnp.where(flip, c_far[at], c_near[at])
                halo[side, q, 8 * t : 8 * t + 8, nz:] = pltpu.roll(tile, 124 - 8 * q, 1)

    def start(a, x):
        layers = WIDE if a == 0 else WIDE - 1
        base = (0, WIDE, 2 * WIDE - 1)[a]
        if x >= nx:
            return halo[0, base + x - nx]
        if x < 0:
            return halo[1, base + layers + x]
        return whole(x, *(u0, r0, w0)[a])

    def span(side, k):
        return (nx - k, nx + SWEEPS - k) if side == 0 else (k - SWEEPS, k)

    def value(side, k, x):
        if k == 0:
            return start(0, x)
        for j, e in enumerate((k, k + 1, nx - 2 - k, nx - 1 - k)):
            if x == e:
                return ends[k - 1][j]
        return steps[k - 1][side, x - span(side, k)[0]]

    for k in range(1, SWEEPS + 1):
        for j in range(SWEEPS):
            for side in (0, 1):
                x = span(side, k)[0] + j
                near = [value(side, k - 1, x + d) for d in (-1, 0, 1)]
                new = stencil(*near, start(1, x), start(2, x))
                reach = SWEEPS - k - max(0, x - nx + 1, -x)
                if k == SWEEPS:
                    last[side, j] = new[:ny, :nz]
                elif reach > 1:
                    steps[k - 1][side, j] = new
                else:
                    steps[k - 1][side, j, :ny, :nz] = new[:ny, :nz]
                    if reach == 1:
                        steps[k - 1][side, j, ny:, :nz] = new[ny:, :nz]
                        steps[k - 1][side, j, :ny, nz:] = new[:ny, nz:]
    for side in (0, 1):
        a, b = span(side, SWEEPS)
        copy = pltpu.make_async_copy(last.at[side], out.at[a:b], sem.at[side])
        copy.start()
        wait.append(copy)
    for copy in wait:
        copy.wait()


def shards(u, r, s):
    nx, ny, nz = u.shape
    cells = nx * ny * nz
    raw = (u, r, s)
    fixed = [pltpu.with_memory_space_constraint(v, pltpu.HBM) for v in raw]
    scratch = [pltpu.VMEM((3, 2, nx, 8, nz), F32), pltpu.SemaphoreType.DMA((3, 2))]
    sent = call(pack_y, [(3, nx // 2, 8, nz)] * 2, fixed, cells // 4, scratch, 8, hbm_in=range(3))
    y = swap(sent, "gy")
    sent = call(pack_z, [(3, nx // 32, ny, 128)] * 2, raw, cells)
    z = swap(sent, "gz")
    sent = call(pack_x, [(len(LAYERS), ny, nz)] * 2, raw, cells // 8)
    x = swap(sent, "gx")
    (w,) = call(weigh, [u.shape], (s,), 8 * cells)
    sent = call(pack_yz, [(3, nx // 32, 8, 128)] * 2, z, cells // 64)
    b = swap(sent, "gy")
    t = call(unpack_z, [(nx, ny, 128)] * 3, z, 8 * cells)
    yy = call(unpack_y, [(nx, 8, nz)] * 3, y, cells)
    shape = (len(LAYERS) + 3, 8, nz)
    *e, c_near, c_far = call(pack_edges, [(nx, 8, 128)] * 3 + [shape] * 2, (*b, *yy, *t), cells // 8)
    c = swap((c_near, c_far), "gx")
    parts = [v for a, m in enumerate((u, r, w)) for v in (m, yy[a], t[a], e[a])]
    block = (ny + 2 * WIDE, nz + 128)
    _, _, first, stop = steps_of(nx)
    scratch = [pltpu.VMEM(u.shape, F32), pltpu.SemaphoreType.DMA] + [pltpu.VMEM((nx,) + block, F32)] * 3
    left = (nx - WIDE - stop + first - WIDE, ny, nz)
    out, rest, *ends = call(
        centre, [u.shape, left] + [(4,) + block] * 3, parts, 60 * cells, scratch, 16, hbm_out=(0,)
    )
    scratch = [
        pltpu.VMEM((2, len(LAYERS)) + block, F32),
        pltpu.VMEM((2, WIDE, ny, nz), F32),
        pltpu.SemaphoreType.DMA((4,)),
    ] + [pltpu.VMEM((2, SWEEPS) + block, F32)] * 3
    operands = (*parts, out, rest, *ends, *x, *c)
    (out,) = call(
        tail, [u.shape], operands, 8 * cells, scratch, 8, hbm_in=(12,), hbm_out=(0,), aliases={12: 0}
    )
    return out


def solution(mesh):
    spec = P("gx", "gy", "gz")
    return jax.shard_map(shards, mesh=mesh, in_specs=(spec,) * 3, out_specs=spec, check_vma=False)
```

```python
import jax
import jax.numpy as jnp
from jax import lax
from jax.experimental import pallas as pl
from jax.experimental.pallas import tpu as pltpu
from jax.sharding import PartitionSpec as P


SWEEPS = 4
WIDE = 4
WEIGHT = 0.8
VMEM = pl.BlockSpec(memory_space=pltpu.VMEM)
HBM = pl.BlockSpec(memory_space=pltpu.HBM)
F32 = jnp.float32
CHUNK = 16
LAYERS = [(a, k) for a, n in enumerate((WIDE, WIDE - 1, WIDE - 1)) for k in range(n)]


def call(kernel, outs, operands, flops, scratch=(), limit=4, hbm_in=(), hbm_out=(), aliases={}):
    return pl.pallas_call(
        kernel,
        out_shape=[jax.ShapeDtypeStruct(s, F32) for s in outs],
        in_specs=[HBM if i in hbm_in else VMEM for i in range(len(operands))],
        out_specs=[HBM if i in hbm_out else VMEM for i in range(len(outs))],
        scratch_shapes=scratch,
        input_output_aliases=aliases,
        compiler_params=pltpu.CompilerParams(vmem_limit_bytes=limit * 2**20),
        cost_estimate=pl.CostEstimate(flops=flops, bytes_accessed=2**20, transcendentals=0),
    )(*operands)


def odd(axis):
    return lax.rem(lax.axis_index(axis), 2)


def swap(sent, axis):
    n = lax.axis_size(axis)
    near = [(i, i ^ 1) for i in range(n)]
    far = [(i, (i + (1 if i % 2 else -1)) % n) for i in range(n)]
    return lax.ppermute(sent[0], axis, near), lax.ppermute(sent[1], axis, far)


def iota(shape, dim):
    return lax.broadcasted_iota(jnp.int32, shape, dim)


def fold(first, second, low):
    row = iota(first.shape, 0)
    keep = jnp.where(low, row, 7 - row) < 4
    return jnp.where(keep, first, pltpu.roll(second, 4, 0))


def unfold(above, below):
    head = iota(above.shape, 0) < 4
    return jnp.where(head, above, below), pltpu.roll(jnp.where(head, below, above), 4, 0)


def pack(u, r, s, u_v, r_v, s_v, y_near, y_far, z_near, z_far, x_near, x_far, sem):
    nx, ny, nz = u.shape
    y_odd, z_odd, x_odd = odd("gy") == 1, odd("gz") == 1, odd("gx") == 1
    held = (u_v, r_v, s_v)
    copies = {}
    for c in range(nx // CHUNK):
        at = pl.ds(c * CHUNK, CHUNK)
        for a, ref in enumerate((u, r, s)):
            copies[c, a] = pltpu.make_async_copy(ref.at[at], held[a].at[at], sem.at[c, a])
            copies[c, a].start()
    block = iota((ny, 128), 1) // 4
    half = iota((ny, 128), 1) < 64
    for c in range(nx // CHUNK):
        for a, ref in enumerate(held):
            copies[c, a].wait()
            for face, low in ((y_near, y_odd), (y_far, jnp.logical_not(y_odd))):
                rows = pl.ds(pl.multiple_of(jnp.where(low, 0, ny - 8), 8), 8)
                for i in range(c * CHUNK // 2, (c + 1) * CHUNK // 2):
                    face[a, i] = fold(ref[2 * i, rows, :], ref[2 * i + 1, rows, :], low)
            g = c * CHUNK // 32
            first = c * CHUNK % 32 == 0
            low = jnp.zeros((ny, 128), F32) if first else z_near[a, g]
            high = jnp.zeros((ny, 128), F32) if first else z_far[a, g]
            low, high = jnp.where(z_odd, low, high), jnp.where(z_odd, high, low)
            for x in range(c * CHUNK, (c + 1) * CHUNK):
                j = x % 32
                both = jnp.where(half, ref[x, :, 0:128], ref[x, :, nz - 128 : nz])
                both = pltpu.roll(both, 4 * j, 1) if j else both
                low = jnp.where(block == j, both, low)
                high = jnp.where(block == (j - 1) % 32, both, high)
            z_near[a, g] = jnp.where(z_odd, low, high)
            z_far[a, g] = jnp.where(z_odd, high, low)
    for face, low in ((x_near, x_odd), (x_far, jnp.logical_not(x_odd))):
        for q, (a, k) in enumerate(LAYERS):
            layers = WIDE if a == 0 else WIDE - 1
            face[q] = held[a][jnp.where(low, k, nx - layers + k)]


def pack_yz(za, zb, near, far):
    ny = za.shape[2]
    is_odd = odd("gy") == 1
    for face, low in ((near, is_odd), (far, jnp.logical_not(is_odd))):
        rows = pl.ds(pl.multiple_of(jnp.where(low, 0, ny - 8), 8), 8)
        for a in range(3):
            for g in range(za.shape[1]):
                face[a, g] = fold(za[a, g, rows, :], zb[a, g, rows, :], low)


def weight(shift):
    return WEIGHT / (6.0 + shift)


def spread_z(high, low, j):
    tile = jnp.where(iota(high.shape, 1) // 4 == j, high, low)
    return pltpu.roll(tile, 128 - 4 * j, 1) if j else tile


def begin(u, r, s, w, part, edge):
    nx, ny, nz = u.shape
    row, lane = iota((ny, nz), 0), iota((ny, nz), 1)
    half = iota((ny, 128), 1) < 64
    w[0] = weight(s[0])
    w[nx - 1] = weight(s[nx - 1])

    def body(i, c):
        for x in (1 + 2 * i, 2 + 2 * i):
            here = u[x]
            beside = u[x - 1] + u[x + 1]
            beside = beside + jnp.where(row == 0, 0.0, pltpu.roll(here, 1, 0))
            beside = beside + jnp.where(row == ny - 1, 0.0, pltpu.roll(here, ny - 1, 0))
            left, right = pltpu.roll(here, 1, 1), pltpu.roll(here, nz - 1, 1)
            edge[x] = jnp.where(half, left[:, :128], right[:, nz - 128 :])
            beside = beside + (jnp.where(lane == 0, 0.0, left) + jnp.where(lane == nz - 1, 0.0, right))
            here_w = weight(s[x])
            w[x] = here_w
            part[x] = 0.2 * here + here_w * (r[x] + beside)
        return c

    lax.fori_loop(0, (nx - 2) // 2, body, 0)


def finish(x, u0, r0, w0, part, edge, new):
    (u, yu, tu, eu), (_, yr, tr, er), (w, yw, tw, ew) = u0, r0, w0
    ny, nz = u.shape[1:]
    row, lane, lane_z = iota((8, nz), 0), iota((ny, 128), 1), iota((8, nz), 1)
    lane_e = iota((8, 128), 1)
    y, t, e = yu[x], tu[x], eu[x]
    t_left, t_right = pltpu.roll(t, 1, 1), pltpu.roll(t, 127, 1)
    e_left, e_right = pltpu.roll(e, 1, 1), pltpu.roll(e, 127, 1)
    y_left, y_right = pltpu.roll(y, 1, 1), pltpu.roll(y, nz - 1, 1)
    y_down, y_up = pltpu.roll(y, 1, 0), pltpu.roll(y, 7, 0)
    halo = jnp.concatenate([jnp.where(lane == 0, t_left, 0.0), jnp.where(lane == 127, t_right, 0.0)], 1)
    halo = jnp.concatenate(
        [
            halo[:8] + jnp.where(row == 0, y_down, 0.0),
            halo[8 : ny - 8],
            halo[ny - 8 :] + jnp.where(row == 7, y_up, 0.0),
        ],
        0,
    )
    new[x, :ny, :nz] = part[x] + w[x] * halo
    beside = yu[x - 1] + yu[x + 1]
    beside = beside + jnp.where(row == 0, pltpu.roll(u[x, ny - 8 :, :], 1, 0), y_down)
    beside = beside + jnp.where(row == 7, pltpu.roll(u[x, :8, :], 7, 0), y_up)
    left = jnp.where(lane_z == 0, jnp.concatenate([e_left, e_left], 1), y_left)
    right = jnp.where(lane_z == nz - 1, jnp.concatenate([e_right, e_right], 1), y_right)
    new[x, ny:, :nz] = 0.2 * y + yw[x] * (yr[x] + (beside + (left + right)))
    column = jnp.concatenate([t, e], 0)
    beside = jnp.concatenate([tu[x - 1] + tu[x + 1], eu[x - 1] + eu[x + 1]], 0)
    beside = beside + (pltpu.roll(column, 1, 0) + pltpu.roll(column, ny + 7, 0))
    left = [jnp.where(lane == 0, edge[x], t_left), jnp.where(lane_e == 0, y_left[:, :128], e_left)]
    right = [jnp.where(lane == 127, edge[x], t_right), jnp.where(lane_e == 127, y_right[:, nz - 128 :], e_right)]
    beside = beside + (jnp.concatenate(left, 0) + jnp.concatenate(right, 0))
    r, w = jnp.concatenate([tr[x], er[x]], 0), jnp.concatenate([tw[x], ew[x]], 0)
    new[x, :, nz:] = 0.2 * column + w * (r + beside)


def spread_z(high, low, j):
    tile = jnp.where(iota(high.shape, 1) // 4 == j, high, low)
    return pltpu.roll(tile, 128 - 4 * j, 1) if j else tile


def unpack_z(za, zb, tu, tr, tw):
    is_odd = odd("gz") == 1
    for a, out in enumerate((tu, tr, tw)):

        def body(g, c, a=a, out=out):
            one, two = za[a, g], zb[a, g]
            high, low = jnp.where(is_odd, two, one), jnp.where(is_odd, one, two)
            for j in range(32):
                tile = spread_z(high, low, j)
                out[g * 32 + j] = weight(tile) if a == 2 else tile
            return c

        lax.fori_loop(0, za.shape[1], body, 0)


def unpack_y(near, far, yu, yr, yw):
    is_odd = odd("gy") == 1
    for a, out in enumerate((yu, yr, yw)):

        def body(i, c, a=a, out=out):
            one, two = near[a, i], far[a, i]
            above, below = jnp.where(is_odd, two, one), jnp.where(is_odd, one, two)
            first, second = unfold(above, below)
            out[2 * i] = weight(first) if a == 2 else first
            out[2 * i + 1] = weight(second) if a == 2 else second
            return c

        lax.fori_loop(0, near.shape[1], body, 0, unroll=4)


def pack_edges(b_near, b_far, yu, yr, yw, tu, tr, tw, eu, er, ew, near, far):
    y_odd, z_odd, x_odd = odd("gy") == 1, odd("gz") == 1, odd("gx") == 1
    for a, out in enumerate((eu, er, ew)):
        for g in range(b_near.shape[1]):
            one, two = b_near[a, g], b_far[a, g]
            above, below = jnp.where(y_odd, two, one), jnp.where(y_odd, one, two)
            first, second = unfold(above, below)
            high, low = jnp.where(z_odd, second, first), jnp.where(z_odd, first, second)
            for j in range(32):
                tile = spread_z(high, low, j)
                out[g * 32 + j] = weight(tile) if a == 2 else tile
    nx = yu.shape[0]
    lane = iota((8, 128), 1) // 8
    for face, low in ((near, x_odd), (far, jnp.logical_not(x_odd))):
        total = [jnp.zeros((8, 128), F32)] * 5
        for q, (a, k) in enumerate(LAYERS):
            layers = WIDE if a == 0 else WIDE - 1
            x = jnp.where(low, k, nx - layers + k)
            face[q] = (yu, yr, yw)[a][x]
            for t in range(5):
                tile = (tu, tr, tw)[a][x, 8 * t : 8 * t + 8, :] if t < 4 else (eu, er, ew)[a][x]
                total[t] = jnp.where(lane == q, pltpu.roll(tile, 8 * q + 4, 1), total[t])
        for t in range(6):
            face[len(LAYERS) + t // 2, :, 128 * (t % 2) : 128 * (t % 2) + 128] = total[min(t, 4)]


def stencil(below, here, above, r, w):
    n, m = here.shape
    beside = below + above
    beside = beside + (pltpu.roll(here, 1, 0) + pltpu.roll(here, n - 1, 0))
    beside = beside + (pltpu.roll(here, 1, 1) + pltpu.roll(here, m - 1, 1))
    return 0.2 * here + w * (r + beside)


def whole(x, main, y, t, e):
    left = jnp.concatenate([main[x], y[x]], 0)
    return jnp.concatenate([left, jnp.concatenate([t[x], e[x]], 0)], 1)


PLANES = 4


def planes(i):
    return [(k, 1 + PLANES * i - k * (PLANES + 1) + j) for k in range(SWEEPS) for j in range(PLANES)]


def steps_of(nx):
    def valid(k, x):
        return k + 1 <= x <= nx - 2 - k

    count = -(-(nx - 1 + (SWEEPS - 1) * (PLANES + 1)) // PLANES)
    done = [[p for p in planes(i) if valid(*p)] for i in range(count)]
    full = [i for i in range(count) if len(done[i]) == SWEEPS * PLANES]
    first = planes(full[0])[-PLANES][1]
    stop = planes(full[-1])[-1][1] + 1
    return done, full, first, stop


def centre(*refs):
    u0, r0, w0 = refs[0:4], refs[4:8], refs[8:12]
    part, edge = refs[12:14]
    out, rest, ends = refs[14], refs[15], refs[16:19]
    last, sem = refs[19:21]
    steps = refs[21:24]
    nx, ny, nz = u0[0].shape
    done, full, first, stop = steps_of(nx)

    def plane(k, x):
        return steps[k - 1][x]

    def one(k, x):
        if k == 0:
            finish(x, u0, r0, w0, part, edge, steps[0])
            return
        r, w = whole(x, *r0), whole(x, *w0)
        new = stencil(plane(k, x - 1), plane(k, x), plane(k, x + 1), r, w)
        if k < SWEEPS - 2:
            steps[k][x] = new
        elif k == SWEEPS - 2:
            steps[k][x, :, :nz] = new[:, :nz]
            steps[k][x, :ny, nz:] = new[:ny, nz:]
        elif isinstance(x, int):
            rest[x - stop if x >= stop else nx - WIDE - stop + x - WIDE] = new[:ny, :nz]
        else:
            last[x] = new[:ny, :nz]

    for i in range(full[0]):
        for p in done[i]:
            one(*p)

    def body(i, c):
        for p in planes(i):
            one(*p)
        at = pl.ds(planes(i)[-PLANES][1], PLANES)
        pltpu.make_async_copy(last.at[at], out.at[at], sem).start()
        return c

    lax.fori_loop(full[0], full[-1] + 1, body, 0)
    for i in range(full[-1] + 1, len(done)):
        for p in done[i]:
            one(*p)
    for k in range(SWEEPS - 1):
        lo, hi = k + 1, nx - 1 - k
        for j, x in enumerate((lo, lo + 1, hi - 2, hi - 1)):
            ends[k][j] = steps[k][x]
    pltpu.make_async_copy(last.at[first:stop], out.at[first:stop], sem).wait()


def tail(*refs):
    u0, r0, w0 = refs[0:4], refs[4:8], refs[8:12]
    rest, ends = refs[13], refs[14:17]
    x_near, x_far, c_near, c_far = refs[17:21]
    out = refs[21]
    halo, last, sem = refs[22:25]
    steps = refs[25:28]
    nx, ny, nz = u0[0].shape
    _, _, first, stop = steps_of(nx)
    wait = []
    if first > WIDE:
        wait.append(pltpu.make_async_copy(rest.at[nx - WIDE - stop :], out.at[WIDE:first], sem.at[2]))
    wait.append(pltpu.make_async_copy(rest.at[: nx - WIDE - stop], out.at[stop : nx - WIDE], sem.at[3]))
    for copy in wait:
        copy.start()
    is_odd = odd("gx") == 1
    for side in (0, 1):
        flip = is_odd if side == 0 else jnp.logical_not(is_odd)
        for q, (a, k) in enumerate(LAYERS):
            main = jnp.where(flip, x_far[q], x_near[q])
            rows = jnp.where(flip, c_far[q], c_near[q])
            put = lambda v: weight(v) if a == 2 else v
            halo[side, q, :ny, :nz] = put(main)
            halo[side, q, ny:, :nz] = rows
            for t in range(5):
                at = (len(LAYERS) + t // 2, slice(None), slice(128 * (t % 2), 128 * (t % 2) + 128))
                tile = jnp.where(flip, c_far[at], c_near[at])
                halo[side, q, 8 * t : 8 * t + 8, nz:] = pltpu.roll(tile, 124 - 8 * q, 1)

    def start(a, x):
        layers = WIDE if a == 0 else WIDE - 1
        base = (0, WIDE, 2 * WIDE - 1)[a]
        if x >= nx:
            return halo[0, base + x - nx]
        if x < 0:
            return halo[1, base + layers + x]
        return whole(x, *(u0, r0, w0)[a])

    def span(side, k):
        return (nx - k, nx + SWEEPS - k) if side == 0 else (k - SWEEPS, k)

    def value(side, k, x):
        if k == 0:
            return start(0, x)
        for j, e in enumerate((k, k + 1, nx - 2 - k, nx - 1 - k)):
            if x == e:
                return ends[k - 1][j]
        return steps[k - 1][side, x - span(side, k)[0]]

    for k in range(1, SWEEPS + 1):
        for j in range(SWEEPS):
            for side in (0, 1):
                x = span(side, k)[0] + j
                near = [value(side, k - 1, x + d) for d in (-1, 0, 1)]
                new = stencil(*near, start(1, x), start(2, x))
                reach = SWEEPS - k - max(0, x - nx + 1, -x)
                if k == SWEEPS:
                    last[side, j] = new[:ny, :nz]
                elif reach > 1:
                    steps[k - 1][side, j] = new
                else:
                    steps[k - 1][side, j, :ny, :nz] = new[:ny, :nz]
                    if reach == 1:
                        steps[k - 1][side, j, ny:, :nz] = new[ny:, :nz]
                        steps[k - 1][side, j, :ny, nz:] = new[:ny, nz:]
    for side in (0, 1):
        a, b = span(side, SWEEPS)
        copy = pltpu.make_async_copy(last.at[side], out.at[a:b], sem.at[side])
        copy.start()
        wait.append(copy)
    for copy in wait:
        copy.wait()


def shards(u, r, s):
    nx, ny, nz = u.shape
    cells = nx * ny * nz
    raw = [pltpu.with_memory_space_constraint(v, pltpu.HBM) for v in (u, r, s)]
    faces = [(3, nx // 2, 8, nz)] * 2 + [(3, nx // 32, ny, 128)] * 2 + [(len(LAYERS), ny, nz)] * 2
    scratch = [pltpu.SemaphoreType.DMA((nx // CHUNK, 3))]
    u, r, s, *sent = call(pack, [u.shape] * 3 + faces, raw, cells // 4, scratch, hbm_in=range(3))
    y = swap(sent[0:2], "gy")
    z = swap(sent[2:4], "gz")
    x = swap(sent[4:6], "gx")
    w, part, edge = call(begin, [u.shape] * 2 + [(nx, ny, 128)], (u, r, s), 20 * cells)
    sent = call(pack_yz, [(3, nx // 32, 8, 128)] * 2, z, cells // 64)
    b = swap(sent, "gy")
    t = call(unpack_z, [(nx, ny, 128)] * 3, z, 8 * cells)
    yy = call(unpack_y, [(nx, 8, nz)] * 3, y, cells)
    shape = (len(LAYERS) + 3, 8, nz)
    *e, c_near, c_far = call(pack_edges, [(nx, 8, 128)] * 3 + [shape] * 2, (*b, *yy, *t), cells // 8)
    c = swap((c_near, c_far), "gx")
    parts = [v for a, m in enumerate((u, r, w)) for v in (m, yy[a], t[a], e[a])]
    block = (ny + 2 * WIDE, nz + 128)
    _, _, first, stop = steps_of(nx)
    scratch = [pltpu.VMEM(u.shape, F32), pltpu.SemaphoreType.DMA] + [pltpu.VMEM((nx,) + block, F32)] * 3
    left = (nx - WIDE - stop + first - WIDE, ny, nz)
    out, rest, *ends = call(
        centre, [u.shape, left] + [(4,) + block] * 3, (*parts, part, edge), 60 * cells, scratch, 16, hbm_out=(0,)
    )
    scratch = [
        pltpu.VMEM((2, len(LAYERS)) + block, F32),
        pltpu.VMEM((2, WIDE, ny, nz), F32),
        pltpu.SemaphoreType.DMA((4,)),
    ] + [pltpu.VMEM((2, SWEEPS) + block, F32)] * 3
    operands = (*parts, out, rest, *ends, *x, *c)
    (out,) = call(
        tail, [u.shape], operands, 8 * cells, scratch, 8, hbm_in=(12,), hbm_out=(0,), aliases={12: 0}
    )
    return out


def solution(mesh):
    spec = P("gx", "gy", "gz")
    return jax.shard_map(shards, mesh=mesh, in_specs=(spec,) * 3, out_specs=spec, check_vma=False)
```

```python
import jax
import jax.numpy as jnp
from jax import lax
from jax.experimental import pallas as pl
from jax.experimental.pallas import tpu as pltpu
from jax.sharding import PartitionSpec as P


SWEEPS = 4
WIDE = 4
WEIGHT = 0.8
VMEM = pl.BlockSpec(memory_space=pltpu.VMEM)
HBM = pl.BlockSpec(memory_space=pltpu.HBM)
F32 = jnp.float32
CHUNK = 16
LAYERS = [(a, k) for a, n in enumerate((WIDE, WIDE - 1, WIDE - 1)) for k in range(n)]


def call(kernel, outs, operands, flops, scratch=(), limit=4, hbm_in=(), hbm_out=(), aliases={}):
    return pl.pallas_call(
        kernel,
        out_shape=[jax.ShapeDtypeStruct(s, F32) for s in outs],
        in_specs=[HBM if i in hbm_in else VMEM for i in range(len(operands))],
        out_specs=[HBM if i in hbm_out else VMEM for i in range(len(outs))],
        scratch_shapes=scratch,
        input_output_aliases=aliases,
        compiler_params=pltpu.CompilerParams(vmem_limit_bytes=limit * 2**20),
        cost_estimate=pl.CostEstimate(flops=flops, bytes_accessed=2**20, transcendentals=0),
    )(*operands)


def odd(axis):
    return lax.rem(lax.axis_index(axis), 2)


def swap(sent, axis):
    n = lax.axis_size(axis)
    near = [(i, i ^ 1) for i in range(n)]
    far = [(i, (i + (1 if i % 2 else -1)) % n) for i in range(n)]
    return lax.ppermute(sent[0], axis, near), lax.ppermute(sent[1], axis, far)


def iota(shape, dim):
    return lax.broadcasted_iota(jnp.int32, shape, dim)


def fold(first, second, low):
    row = iota(first.shape, 0)
    keep = jnp.where(low, row, 7 - row) < 4
    return jnp.where(keep, first, pltpu.roll(second, 4, 0))


def unfold(above, below):
    head = iota(above.shape, 0) < 4
    return jnp.where(head, above, below), pltpu.roll(jnp.where(head, below, above), 4, 0)


def pack(u, r, s, u_v, r_v, s_v, y_near, y_far, z_near, z_far, x_near, x_far, sem):
    nx, ny, nz = u.shape
    y_odd, z_odd, x_odd = odd("gy") == 1, odd("gz") == 1, odd("gx") == 1
    held = (u_v, r_v, s_v)
    copies = {}
    for c in range(nx // CHUNK):
        at = pl.ds(c * CHUNK, CHUNK)
        for a, ref in enumerate((u, r, s)):
            copies[c, a] = pltpu.make_async_copy(ref.at[at], held[a].at[at], sem.at[c, a])
            copies[c, a].start()
    block = iota((ny, 128), 1) // 4
    half = iota((ny, 128), 1) < 64
    for c in range(nx // CHUNK):
        for a, ref in enumerate(held):
            copies[c, a].wait()
            for face, low in ((y_near, y_odd), (y_far, jnp.logical_not(y_odd))):
                rows = pl.ds(pl.multiple_of(jnp.where(low, 0, ny - 8), 8), 8)
                for i in range(c * CHUNK // 2, (c + 1) * CHUNK // 2):
                    face[a, i] = fold(ref[2 * i, rows, :], ref[2 * i + 1, rows, :], low)
            g = c * CHUNK // 32
            first = c * CHUNK % 32 == 0
            low = jnp.zeros((ny, 128), F32) if first else z_near[a, g]
            high = jnp.zeros((ny, 128), F32) if first else z_far[a, g]
            low, high = jnp.where(z_odd, low, high), jnp.where(z_odd, high, low)
            for x in range(c * CHUNK, (c + 1) * CHUNK):
                j = x % 32
                both = jnp.where(half, ref[x, :, 0:128], ref[x, :, nz - 128 : nz])
                both = pltpu.roll(both, 4 * j, 1) if j else both
                low = jnp.where(block == j, both, low)
                high = jnp.where(block == (j - 1) % 32, both, high)
            z_near[a, g] = jnp.where(z_odd, low, high)
            z_far[a, g] = jnp.where(z_odd, high, low)
    for face, low in ((x_near, x_odd), (x_far, jnp.logical_not(x_odd))):
        for q, (a, k) in enumerate(LAYERS):
            layers = WIDE if a == 0 else WIDE - 1
            face[q] = held[a][jnp.where(low, k, nx - layers + k)]


def pack_yz(za, zb, near, far):
    ny = za.shape[2]
    is_odd = odd("gy") == 1
    for face, low in ((near, is_odd), (far, jnp.logical_not(is_odd))):
        rows = pl.ds(pl.multiple_of(jnp.where(low, 0, ny - 8), 8), 8)
        for a in range(3):
            for g in range(za.shape[1]):
                face[a, g] = fold(za[a, g, rows, :], zb[a, g, rows, :], low)


def weight(shift):
    return WEIGHT / (6.0 + shift)


def spread_z(high, low, j):
    tile = jnp.where(iota(high.shape, 1) // 4 == j, high, low)
    return pltpu.roll(tile, 128 - 4 * j, 1) if j else tile


def begin(u, r, s, w, part, edge):
    nx, ny, nz = u.shape
    row, lane = iota((ny, nz), 0), iota((ny, nz), 1)
    half = iota((ny, 128), 1) < 64

    def body(i, c):
        for j in range(8):
            x = 8 * i + j
            here = u[x]
            beside = u[jnp.maximum(x - 1, 0)] + u[jnp.minimum(x + 1, nx - 1)]
            beside = beside + jnp.where(row == 0, 0.0, pltpu.roll(here, 1, 0))
            beside = beside + jnp.where(row == ny - 1, 0.0, pltpu.roll(here, ny - 1, 0))
            left, right = pltpu.roll(here, 1, 1), pltpu.roll(here, nz - 1, 1)
            edge[x] = jnp.where(half, left[:, :128], right[:, nz - 128 :])
            beside = beside + (jnp.where(lane == 0, 0.0, left) + jnp.where(lane == nz - 1, 0.0, right))
            here_w = weight(s[x])
            w[x] = here_w
            part[x] = 0.2 * here + here_w * (r[x] + beside)
        return c

    lax.fori_loop(0, nx // 8, body, 0)


def finish(x, u0, r0, w0, part, edge, new):
    (u, yu, tu, eu), (_, yr, tr, er), (w, yw, tw, ew) = u0, r0, w0
    ny, nz = u.shape[1:]
    row, lane, lane_z = iota((8, nz), 0), iota((ny, 128), 1), iota((8, nz), 1)
    lane_e = iota((8, 128), 1)
    y, t, e = yu[x], tu[x], eu[x]
    t_left, t_right = pltpu.roll(t, 1, 1), pltpu.roll(t, 127, 1)
    e_left, e_right = pltpu.roll(e, 1, 1), pltpu.roll(e, 127, 1)
    y_left, y_right = pltpu.roll(y, 1, 1), pltpu.roll(y, nz - 1, 1)
    y_down, y_up = pltpu.roll(y, 1, 0), pltpu.roll(y, 7, 0)
    halo = jnp.concatenate([jnp.where(lane == 0, t_left, 0.0), jnp.where(lane == 127, t_right, 0.0)], 1)
    halo = jnp.concatenate(
        [
            halo[:8] + jnp.where(row == 0, y_down, 0.0),
            halo[8 : ny - 8],
            halo[ny - 8 :] + jnp.where(row == 7, y_up, 0.0),
        ],
        0,
    )
    new[x, :ny, :nz] = part[x] + w[x] * halo
    beside = yu[x - 1] + yu[x + 1]
    beside = beside + jnp.where(row == 0, pltpu.roll(u[x, ny - 8 :, :], 1, 0), y_down)
    beside = beside + jnp.where(row == 7, pltpu.roll(u[x, :8, :], 7, 0), y_up)
    left = jnp.where(lane_z == 0, jnp.concatenate([e_left, e_left], 1), y_left)
    right = jnp.where(lane_z == nz - 1, jnp.concatenate([e_right, e_right], 1), y_right)
    new[x, ny:, :nz] = 0.2 * y + yw[x] * (yr[x] + (beside + (left + right)))
    column = jnp.concatenate([t, e], 0)
    beside = jnp.concatenate([tu[x - 1] + tu[x + 1], eu[x - 1] + eu[x + 1]], 0)
    beside = beside + (pltpu.roll(column, 1, 0) + pltpu.roll(column, ny + 7, 0))
    left = [jnp.where(lane == 0, edge[x], t_left), jnp.where(lane_e == 0, y_left[:, :128], e_left)]
    right = [jnp.where(lane == 127, edge[x], t_right), jnp.where(lane_e == 127, y_right[:, nz - 128 :], e_right)]
    beside = beside + (jnp.concatenate(left, 0) + jnp.concatenate(right, 0))
    r, w = jnp.concatenate([tr[x], er[x]], 0), jnp.concatenate([tw[x], ew[x]], 0)
    new[x, :, nz:] = 0.2 * column + w * (r + beside)


def spread_z(high, low, j):
    tile = jnp.where(iota(high.shape, 1) // 4 == j, high, low)
    return pltpu.roll(tile, 128 - 4 * j, 1) if j else tile


def unpack_z(za, zb, tu, tr, tw):
    is_odd = odd("gz") == 1
    for a, out in enumerate((tu, tr, tw)):

        def body(g, c, a=a, out=out):
            one, two = za[a, g], zb[a, g]
            high, low = jnp.where(is_odd, two, one), jnp.where(is_odd, one, two)
            for j in range(32):
                tile = spread_z(high, low, j)
                out[g * 32 + j] = weight(tile) if a == 2 else tile
            return c

        lax.fori_loop(0, za.shape[1], body, 0)


def unpack_y(near, far, yu, yr, yw):
    is_odd = odd("gy") == 1
    for a, out in enumerate((yu, yr, yw)):

        def body(i, c, a=a, out=out):
            one, two = near[a, i], far[a, i]
            above, below = jnp.where(is_odd, two, one), jnp.where(is_odd, one, two)
            first, second = unfold(above, below)
            out[2 * i] = weight(first) if a == 2 else first
            out[2 * i + 1] = weight(second) if a == 2 else second
            return c

        lax.fori_loop(0, near.shape[1], body, 0, unroll=4)


def pack_edges(b_near, b_far, yu, yr, yw, tu, tr, tw, eu, er, ew, near, far):
    y_odd, z_odd, x_odd = odd("gy") == 1, odd("gz") == 1, odd("gx") == 1
    for a, out in enumerate((eu, er, ew)):
        for g in range(b_near.shape[1]):
            one, two = b_near[a, g], b_far[a, g]
            above, below = jnp.where(y_odd, two, one), jnp.where(y_odd, one, two)
            first, second = unfold(above, below)
            high, low = jnp.where(z_odd, second, first), jnp.where(z_odd, first, second)
            for j in range(32):
                tile = spread_z(high, low, j)
                out[g * 32 + j] = weight(tile) if a == 2 else tile
    nx = yu.shape[0]
    lane = iota((8, 128), 1) // 8
    for face, low in ((near, x_odd), (far, jnp.logical_not(x_odd))):
        total = [jnp.zeros((8, 128), F32)] * 5
        for q, (a, k) in enumerate(LAYERS):
            layers = WIDE if a == 0 else WIDE - 1
            x = jnp.where(low, k, nx - layers + k)
            face[q] = (yu, yr, yw)[a][x]
            for t in range(5):
                tile = (tu, tr, tw)[a][x, 8 * t : 8 * t + 8, :] if t < 4 else (eu, er, ew)[a][x]
                total[t] = jnp.where(lane == q, pltpu.roll(tile, 8 * q + 4, 1), total[t])
        for t in range(6):
            face[len(LAYERS) + t // 2, :, 128 * (t % 2) : 128 * (t % 2) + 128] = total[min(t, 4)]


def stencil(below, here, above, r, w):
    n, m = here.shape
    beside = below + above
    beside = beside + (pltpu.roll(here, 1, 0) + pltpu.roll(here, n - 1, 0))
    beside = beside + (pltpu.roll(here, 1, 1) + pltpu.roll(here, m - 1, 1))
    return 0.2 * here + w * (r + beside)


def whole(x, main, y, t, e):
    left = jnp.concatenate([main[x], y[x]], 0)
    return jnp.concatenate([left, jnp.concatenate([t[x], e[x]], 0)], 1)


PLANES = 4


def planes(i):
    return [(k, 1 + PLANES * i - k * (PLANES + 1) + j) for k in range(SWEEPS) for j in range(PLANES)]


def steps_of(nx):
    def valid(k, x):
        return k + 1 <= x <= nx - 2 - k

    count = -(-(nx - 1 + (SWEEPS - 1) * (PLANES + 1)) // PLANES)
    done = [[p for p in planes(i) if valid(*p)] for i in range(count)]
    full = [i for i in range(count) if len(done[i]) == SWEEPS * PLANES]
    first = planes(full[0])[-PLANES][1]
    stop = planes(full[-1])[-1][1] + 1
    return done, full, first, stop


def centre(*refs):
    u0, r0, w0 = refs[0:4], refs[4:8], refs[8:12]
    part, edge = refs[12:14]
    out, rest, ends = refs[14], refs[15], refs[16:19]
    last, sem = refs[19:21]
    steps = refs[21:24]
    nx, ny, nz = u0[0].shape
    done, full, first, stop = steps_of(nx)

    def plane(k, x):
        return steps[k - 1][x]

    def one(k, x):
        if k == 0:
            finish(x, u0, r0, w0, part, edge, steps[0])
            return
        r, w = whole(x, *r0), whole(x, *w0)
        new = stencil(plane(k, x - 1), plane(k, x), plane(k, x + 1), r, w)
        if k < SWEEPS - 2:
            steps[k][x] = new
        elif k == SWEEPS - 2:
            steps[k][x, :, :nz] = new[:, :nz]
            steps[k][x, :ny, nz:] = new[:ny, nz:]
        elif isinstance(x, int):
            rest[x - stop if x >= stop else nx - WIDE - stop + x - WIDE] = new[:ny, :nz]
        else:
            last[x] = new[:ny, :nz]

    for i in range(full[0]):
        for p in done[i]:
            one(*p)

    def body(i, c):
        for p in planes(i):
            one(*p)
        at = pl.ds(planes(i)[-PLANES][1], PLANES)
        pltpu.make_async_copy(last.at[at], out.at[at], sem).start()
        return c

    lax.fori_loop(full[0], full[-1] + 1, body, 0)
    for i in range(full[-1] + 1, len(done)):
        for p in done[i]:
            one(*p)
    for k in range(SWEEPS - 1):
        lo, hi = k + 1, nx - 1 - k
        for j, x in enumerate((lo, lo + 1, hi - 2, hi - 1)):
            ends[k][j] = steps[k][x]
    pltpu.make_async_copy(last.at[first:stop], out.at[first:stop], sem).wait()


def tail(*refs):
    u0, r0, w0 = refs[0:4], refs[4:8], refs[8:12]
    rest, ends = refs[13], refs[14:17]
    x_near, x_far, c_near, c_far = refs[17:21]
    out = refs[21]
    halo, last, sem = refs[22:25]
    steps = refs[25:28]
    nx, ny, nz = u0[0].shape
    _, _, first, stop = steps_of(nx)
    wait = []
    if first > WIDE:
        wait.append(pltpu.make_async_copy(rest.at[nx - WIDE - stop :], out.at[WIDE:first], sem.at[2]))
    wait.append(pltpu.make_async_copy(rest.at[: nx - WIDE - stop], out.at[stop : nx - WIDE], sem.at[3]))
    for copy in wait:
        copy.start()
    is_odd = odd("gx") == 1
    for side in (0, 1):
        flip = is_odd if side == 0 else jnp.logical_not(is_odd)
        for q, (a, k) in enumerate(LAYERS):
            main = jnp.where(flip, x_far[q], x_near[q])
            rows = jnp.where(flip, c_far[q], c_near[q])
            put = lambda v: weight(v) if a == 2 else v
            halo[side, q, :ny, :nz] = put(main)
            halo[side, q, ny:, :nz] = rows
            for t in range(5):
                at = (len(LAYERS) + t // 2, slice(None), slice(128 * (t % 2), 128 * (t % 2) + 128))
                tile = jnp.where(flip, c_far[at], c_near[at])
                halo[side, q, 8 * t : 8 * t + 8, nz:] = pltpu.roll(tile, 124 - 8 * q, 1)

    def start(a, x):
        layers = WIDE if a == 0 else WIDE - 1
        base = (0, WIDE, 2 * WIDE - 1)[a]
        if x >= nx:
            return halo[0, base + x - nx]
        if x < 0:
            return halo[1, base + layers + x]
        return whole(x, *(u0, r0, w0)[a])

    def span(side, k):
        return (nx - k, nx + SWEEPS - k) if side == 0 else (k - SWEEPS, k)

    def value(side, k, x):
        if k == 0:
            return start(0, x)
        for j, e in enumerate((k, k + 1, nx - 2 - k, nx - 1 - k)):
            if x == e:
                return ends[k - 1][j]
        return steps[k - 1][side, x - span(side, k)[0]]

    for k in range(1, SWEEPS + 1):
        for j in range(SWEEPS):
            for side in (0, 1):
                x = span(side, k)[0] + j
                near = [value(side, k - 1, x + d) for d in (-1, 0, 1)]
                new = stencil(*near, start(1, x), start(2, x))
                reach = SWEEPS - k - max(0, x - nx + 1, -x)
                if k == SWEEPS:
                    last[side, j] = new[:ny, :nz]
                elif reach > 1:
                    steps[k - 1][side, j] = new
                else:
                    steps[k - 1][side, j, :ny, :nz] = new[:ny, :nz]
                    if reach == 1:
                        steps[k - 1][side, j, ny:, :nz] = new[ny:, :nz]
                        steps[k - 1][side, j, :ny, nz:] = new[:ny, nz:]
    for side in (0, 1):
        a, b = span(side, SWEEPS)
        copy = pltpu.make_async_copy(last.at[side], out.at[a:b], sem.at[side])
        copy.start()
        wait.append(copy)
    for copy in wait:
        copy.wait()


def shards(u, r, s):
    nx, ny, nz = u.shape
    cells = nx * ny * nz
    raw = [pltpu.with_memory_space_constraint(v, pltpu.HBM) for v in (u, r, s)]
    faces = [(3, nx // 2, 8, nz)] * 2 + [(3, nx // 32, ny, 128)] * 2 + [(len(LAYERS), ny, nz)] * 2
    scratch = [pltpu.SemaphoreType.DMA((nx // CHUNK, 3))]
    u, r, s, *sent = call(pack, [u.shape] * 3 + faces, raw, cells // 4, scratch, hbm_in=range(3))
    y = swap(sent[0:2], "gy")
    z = swap(sent[2:4], "gz")
    x = swap(sent[4:6], "gx")
    w, part, edge = call(begin, [u.shape] * 2 + [(nx, ny, 128)], (u, r, s), 20 * cells)
    sent = call(pack_yz, [(3, nx // 32, 8, 128)] * 2, z, cells // 64)
    b = swap(sent, "gy")
    t = call(unpack_z, [(nx, ny, 128)] * 3, z, 8 * cells)
    yy = call(unpack_y, [(nx, 8, nz)] * 3, y, cells)
    shape = (len(LAYERS) + 3, 8, nz)
    *e, c_near, c_far = call(pack_edges, [(nx, 8, 128)] * 3 + [shape] * 2, (*b, *yy, *t), cells // 8)
    c = swap((c_near, c_far), "gx")
    parts = [v for a, m in enumerate((u, r, w)) for v in (m, yy[a], t[a], e[a])]
    block = (ny + 2 * WIDE, nz + 128)
    _, _, first, stop = steps_of(nx)
    scratch = [pltpu.VMEM(u.shape, F32), pltpu.SemaphoreType.DMA] + [pltpu.VMEM((nx,) + block, F32)] * 3
    left = (nx - WIDE - stop + first - WIDE, ny, nz)
    out, rest, *ends = call(
        centre, [u.shape, left] + [(4,) + block] * 3, (*parts, part, edge), 60 * cells, scratch, 16, hbm_out=(0,)
    )
    scratch = [
        pltpu.VMEM((2, len(LAYERS)) + block, F32),
        pltpu.VMEM((2, WIDE, ny, nz), F32),
        pltpu.SemaphoreType.DMA((4,)),
    ] + [pltpu.VMEM((2, SWEEPS) + block, F32)] * 3
    operands = (*parts, out, rest, *ends, *x, *c)
    (out,) = call(
        tail, [u.shape], operands, 8 * cells, scratch, 8, hbm_in=(12,), hbm_out=(0,), aliases={12: 0}
    )
    return out


def solution(mesh):
    spec = P("gx", "gy", "gz")
    return jax.shard_map(shards, mesh=mesh, in_specs=(spec,) * 3, out_specs=spec, check_vma=False)
```

```python
import jax
import jax.numpy as jnp
from jax import lax
from jax.experimental import pallas as pl
from jax.experimental.pallas import tpu as pltpu
from jax.sharding import PartitionSpec as P


SWEEPS = 4
WIDE = 4
WEIGHT = 0.8
VMEM = pl.BlockSpec(memory_space=pltpu.VMEM)
HBM = pl.BlockSpec(memory_space=pltpu.HBM)
F32 = jnp.float32
CHUNK = 16
LAYERS = [(a, k) for a, n in enumerate((WIDE, WIDE - 1, WIDE - 1)) for k in range(n)]


def call(kernel, outs, operands, flops, scratch=(), limit=4, hbm_in=(), hbm_out=(), aliases={}):
    return pl.pallas_call(
        kernel,
        out_shape=[jax.ShapeDtypeStruct(s, F32) for s in outs],
        in_specs=[HBM if i in hbm_in else VMEM for i in range(len(operands))],
        out_specs=[HBM if i in hbm_out else VMEM for i in range(len(outs))],
        scratch_shapes=scratch,
        input_output_aliases=aliases,
        compiler_params=pltpu.CompilerParams(vmem_limit_bytes=limit * 2**20),
        cost_estimate=pl.CostEstimate(flops=flops, bytes_accessed=2**20, transcendentals=0),
    )(*operands)


def odd(axis):
    return lax.rem(lax.axis_index(axis), 2)


def swap(sent, axis):
    n = lax.axis_size(axis)
    near = [(i, i ^ 1) for i in range(n)]
    far = [(i, (i + (1 if i % 2 else -1)) % n) for i in range(n)]
    got = lax.ppermute(sent[1], axis, far)
    return lax.ppermute(sent[0], axis, near), got


def iota(shape, dim):
    return lax.broadcasted_iota(jnp.int32, shape, dim)


def fold(first, second, low):
    row = iota(first.shape, 0)
    keep = jnp.where(low, row, 7 - row) < 4
    return jnp.where(keep, first, pltpu.roll(second, 4, 0))


def unfold(above, below):
    head = iota(above.shape, 0) < 4
    return jnp.where(head, above, below), pltpu.roll(jnp.where(head, below, above), 4, 0)


def turn(tile, n):
    return pltpu.roll(tile, n % 8, 0) if n % 8 else tile


def fold_rows(held, x, at):
    row = iota((8, held[0].shape[2]), 0)
    tiles, rest = [], None
    for k in range(4):
        u, r, s = (ref[x + k, at : at + 8, :] for ref in held)
        if at == 0:
            tiles.append(jnp.where(row < 4, u, jnp.where(row < 7, turn(r, 4), turn(s, 7))))
            two = turn(s, 2 * k - 1)
        else:
            tiles.append(jnp.where(row > 3, u, jnp.where(row > 0, turn(r, 4), turn(s, 1))))
            two = turn(s, 2 * k - 5)
        rest = two if k == 0 else jnp.where(row // 2 == k, two, rest)
    return tiles + [rest]


def pack(u, r, s, u_v, r_v, s_v, y_near, y_far, z_near, z_far, x_near, x_far, sem):
    nx, ny, nz = u.shape
    y_odd, z_odd, x_odd = odd("gy") == 1, odd("gz") == 1, odd("gx") == 1
    held = (u_v, r_v, s_v)
    copies = {}
    for c in range(nx // CHUNK):
        at = pl.ds(c * CHUNK, CHUNK)
        for a, ref in enumerate((u, r, s)):
            copies[c, a] = pltpu.make_async_copy(ref.at[at], held[a].at[at], sem.at[c, a])
            copies[c, a].start()
    block = iota((ny, 128), 1) // 4
    half = iota((ny, 128), 1) < 64
    for c in range(nx // CHUNK):
        for a, ref in enumerate(held):
            copies[c, a].wait()
            g = c * CHUNK // 32
            first = c * CHUNK % 32 == 0
            low = jnp.zeros((ny, 128), F32) if first else z_near[a, g]
            high = jnp.zeros((ny, 128), F32) if first else z_far[a, g]
            low, high = jnp.where(z_odd, low, high), jnp.where(z_odd, high, low)
            for x in range(c * CHUNK, (c + 1) * CHUNK):
                j = x % 32
                both = jnp.where(half, ref[x, :, 0:128], ref[x, :, nz - 128 : nz])
                both = pltpu.roll(both, 4 * j, 1) if j else both
                low = jnp.where(block == j, both, low)
                high = jnp.where(block == (j - 1) % 32, both, high)
            z_near[a, g] = jnp.where(z_odd, low, high)
            z_far[a, g] = jnp.where(z_odd, high, low)
        for i in range(c * CHUNK // 4, (c + 1) * CHUNK // 4):
            low, high = fold_rows(held, 4 * i, 0), fold_rows(held, 4 * i, ny - 8)
            for n in range(5):
                y_near[i, n] = jnp.where(y_odd, low[n], high[n])
                y_far[i, n] = jnp.where(y_odd, high[n], low[n])
    for face, low in ((x_near, x_odd), (x_far, jnp.logical_not(x_odd))):
        for q, (a, k) in enumerate(LAYERS):
            layers = WIDE if a == 0 else WIDE - 1
            face[q] = held[a][jnp.where(low, k, nx - layers + k)]


def pack_yz(za, zb, near, far):
    ny = za.shape[2]
    is_odd = odd("gy") == 1
    for face, low in ((near, is_odd), (far, jnp.logical_not(is_odd))):
        rows = pl.ds(pl.multiple_of(jnp.where(low, 0, ny - 8), 8), 8)
        for a in range(3):
            for g in range(za.shape[1]):
                face[a, g] = fold(za[a, g, rows, :], zb[a, g, rows, :], low)


def weight(shift):
    return WEIGHT / (6.0 + shift)


def spread_z(high, low, j):
    tile = jnp.where(iota(high.shape, 1) // 4 == j, high, low)
    return pltpu.roll(tile, 128 - 4 * j, 1) if j else tile


def begin(u, r, s, w, part, edge):
    nx, ny, nz = u.shape
    row, lane = iota((ny, nz), 0), iota((ny, nz), 1)
    half = iota((ny, 128), 1) < 64

    def body(i, c):
        for j in range(8):
            x = 8 * i + j
            here = u[x]
            beside = u[jnp.maximum(x - 1, 0)] + u[jnp.minimum(x + 1, nx - 1)]
            beside = beside + jnp.where(row == 0, 0.0, pltpu.roll(here, 1, 0))
            beside = beside + jnp.where(row == ny - 1, 0.0, pltpu.roll(here, ny - 1, 0))
            left, right = pltpu.roll(here, 1, 1), pltpu.roll(here, nz - 1, 1)
            edge[x] = jnp.where(half, left[:, :128], right[:, nz - 128 :])
            beside = beside + (jnp.where(lane == 0, 0.0, left) + jnp.where(lane == nz - 1, 0.0, right))
            here_w = weight(s[x])
            w[x] = here_w
            part[x] = 0.2 * here + here_w * (r[x] + beside)
        return c

    lax.fori_loop(0, nx // 8, body, 0)


def finish(x, u0, r0, w0, part, edge, new):
    (u, yu, tu, eu), (_, yr, tr, er), (w, yw, tw, ew) = u0, r0, w0
    ny, nz = u.shape[1:]
    row, lane, lane_z = iota((8, nz), 0), iota((ny, 128), 1), iota((8, nz), 1)
    lane_e = iota((8, 128), 1)
    y, t, e = yu[x], tu[x], eu[x]
    t_left, t_right = pltpu.roll(t, 1, 1), pltpu.roll(t, 127, 1)
    e_left, e_right = pltpu.roll(e, 1, 1), pltpu.roll(e, 127, 1)
    y_left, y_right = pltpu.roll(y, 1, 1), pltpu.roll(y, nz - 1, 1)
    y_down, y_up = pltpu.roll(y, 1, 0), pltpu.roll(y, 7, 0)
    halo = jnp.concatenate([jnp.where(lane == 0, t_left, 0.0), jnp.where(lane == 127, t_right, 0.0)], 1)
    halo = jnp.concatenate(
        [
            halo[:8] + jnp.where(row == 0, y_down, 0.0),
            halo[8 : ny - 8],
            halo[ny - 8 :] + jnp.where(row == 7, y_up, 0.0),
        ],
        0,
    )
    new[x, :ny, :nz] = part[x] + w[x] * halo
    beside = yu[x - 1] + yu[x + 1]
    beside = beside + jnp.where(row == 0, pltpu.roll(u[x, ny - 8 :, :], 1, 0), y_down)
    beside = beside + jnp.where(row == 7, pltpu.roll(u[x, :8, :], 7, 0), y_up)
    left = jnp.where(lane_z == 0, jnp.concatenate([e_left, e_left], 1), y_left)
    right = jnp.where(lane_z == nz - 1, jnp.concatenate([e_right, e_right], 1), y_right)
    new[x, ny:, :nz] = 0.2 * y + yw[x] * (yr[x] + (beside + (left + right)))
    column = jnp.concatenate([t, e], 0)
    beside = jnp.concatenate([tu[x - 1] + tu[x + 1], eu[x - 1] + eu[x + 1]], 0)
    beside = beside + (pltpu.roll(column, 1, 0) + pltpu.roll(column, ny + 7, 0))
    left = [jnp.where(lane == 0, edge[x], t_left), jnp.where(lane_e == 0, y_left[:, :128], e_left)]
    right = [jnp.where(lane == 127, edge[x], t_right), jnp.where(lane_e == 127, y_right[:, nz - 128 :], e_right)]
    beside = beside + (jnp.concatenate(left, 0) + jnp.concatenate(right, 0))
    r, w = jnp.concatenate([tr[x], er[x]], 0), jnp.concatenate([tw[x], ew[x]], 0)
    new[x, :, nz:] = 0.2 * column + w * (r + beside)


def spread_z(high, low, j):
    tile = jnp.where(iota(high.shape, 1) // 4 == j, high, low)
    return pltpu.roll(tile, 128 - 4 * j, 1) if j else tile


def unpack_z(za, zb, tu, tr, tw):
    is_odd = odd("gz") == 1
    for a, out in enumerate((tu, tr, tw)):

        def body(g, c, a=a, out=out):
            one, two = za[a, g], zb[a, g]
            high, low = jnp.where(is_odd, two, one), jnp.where(is_odd, one, two)
            for j in range(32):
                tile = spread_z(high, low, j)
                out[g * 32 + j] = weight(tile) if a == 2 else tile
            return c

        lax.fori_loop(0, za.shape[1], body, 0)


def unpack_y(near, far, yu, yr, yw):
    is_odd = odd("gy") == 1
    row = iota(near.shape[2:], 0)

    def body(i, c):
        def halves(n):
            one, two = near[i, n], far[i, n]
            return jnp.where(is_odd, two, one), jnp.where(is_odd, one, two)

        rest_above, rest_below = halves(4)
        for k in range(4):
            above, below = halves(k)
            yu[4 * i + k] = jnp.where(row < 4, above, below)
            yr[4 * i + k] = turn(jnp.where(row < 4, below, above), 4)
            s = jnp.where(row < 4, turn(rest_above, 1 - 2 * k), turn(rest_below, 5 - 2 * k))
            s = jnp.where(row == 0, turn(above, 1), jnp.where(row == 7, turn(below, 7), s))
            yw[4 * i + k] = weight(s)
        return c

    lax.fori_loop(0, near.shape[0], body, 0, unroll=2)


def pack_edges(b_near, b_far, yu, yr, yw, tu, tr, tw, eu, er, ew, near, far):
    y_odd, z_odd, x_odd = odd("gy") == 1, odd("gz") == 1, odd("gx") == 1
    for a, out in enumerate((eu, er, ew)):
        for g in range(b_near.shape[1]):
            one, two = b_near[a, g], b_far[a, g]
            above, below = jnp.where(y_odd, two, one), jnp.where(y_odd, one, two)
            first, second = unfold(above, below)
            high, low = jnp.where(z_odd, second, first), jnp.where(z_odd, first, second)
            for j in range(32):
                tile = spread_z(high, low, j)
                out[g * 32 + j] = weight(tile) if a == 2 else tile
    nx = yu.shape[0]
    lane = iota((8, 128), 1) // 8
    for face, low in ((near, x_odd), (far, jnp.logical_not(x_odd))):
        total = [jnp.zeros((8, 128), F32)] * 5
        for q, (a, k) in enumerate(LAYERS):
            layers = WIDE if a == 0 else WIDE - 1
            x = jnp.where(low, k, nx - layers + k)
            face[q] = (yu, yr, yw)[a][x]
            for t in range(5):
                tile = (tu, tr, tw)[a][x, 8 * t : 8 * t + 8, :] if t < 4 else (eu, er, ew)[a][x]
                total[t] = jnp.where(lane == q, pltpu.roll(tile, 8 * q + 4, 1), total[t])
        for t in range(6):
            face[len(LAYERS) + t // 2, :, 128 * (t % 2) : 128 * (t % 2) + 128] = total[min(t, 4)]


def stencil(below, here, above, r, w):
    n, m = here.shape
    beside = below + above
    beside = beside + (pltpu.roll(here, 1, 0) + pltpu.roll(here, n - 1, 0))
    beside = beside + (pltpu.roll(here, 1, 1) + pltpu.roll(here, m - 1, 1))
    return 0.2 * here + w * (r + beside)


def whole(x, main, y, t, e):
    left = jnp.concatenate([main[x], y[x]], 0)
    return jnp.concatenate([left, jnp.concatenate([t[x], e[x]], 0)], 1)


PLANES = 4


def planes(i):
    return [(k, 1 + PLANES * i - k * (PLANES + 1) + j) for k in range(SWEEPS) for j in range(PLANES)]


def steps_of(nx):
    def valid(k, x):
        return k + 1 <= x <= nx - 2 - k

    count = -(-(nx - 1 + (SWEEPS - 1) * (PLANES + 1)) // PLANES)
    done = [[p for p in planes(i) if valid(*p)] for i in range(count)]
    full = [i for i in range(count) if len(done[i]) == SWEEPS * PLANES]
    first = planes(full[0])[-PLANES][1]
    stop = planes(full[-1])[-1][1] + 1
    return done, full, first, stop


def centre(*refs):
    u0, r0, w0 = refs[0:4], refs[4:8], refs[8:12]
    part, edge = refs[12:14]
    out, rest, ends = refs[14], refs[15], refs[16:19]
    last, sem = refs[19:21]
    steps = refs[21:24]
    nx, ny, nz = u0[0].shape
    done, full, first, stop = steps_of(nx)

    def plane(k, x):
        return steps[k - 1][x]

    def one(k, x):
        if k == 0:
            finish(x, u0, r0, w0, part, edge, steps[0])
            return
        r, w = whole(x, *r0), whole(x, *w0)
        new = stencil(plane(k, x - 1), plane(k, x), plane(k, x + 1), r, w)
        if k < SWEEPS - 2:
            steps[k][x] = new
        elif k == SWEEPS - 2:
            steps[k][x, :, :nz] = new[:, :nz]
            steps[k][x, :ny, nz:] = new[:ny, nz:]
        elif isinstance(x, int):
            rest[x - stop if x >= stop else nx - WIDE - stop + x - WIDE] = new[:ny, :nz]
        else:
            last[x] = new[:ny, :nz]

    for i in range(full[0]):
        for p in done[i]:
            one(*p)

    def body(i, c):
        for p in planes(i):
            one(*p)
        at = pl.ds(planes(i)[-PLANES][1], PLANES)
        pltpu.make_async_copy(last.at[at], out.at[at], sem).start()
        return c

    lax.fori_loop(full[0], full[-1] + 1, body, 0)
    for i in range(full[-1] + 1, len(done)):
        for p in done[i]:
            one(*p)
    for k in range(SWEEPS - 1):
        lo, hi = k + 1, nx - 1 - k
        for j, x in enumerate((lo, lo + 1, hi - 2, hi - 1)):
            ends[k][j] = steps[k][x]
    pltpu.make_async_copy(last.at[first:stop], out.at[first:stop], sem).wait()


def tail(*refs):
    u0, r0, w0 = refs[0:4], refs[4:8], refs[8:12]
    rest, ends = refs[13], refs[14:17]
    x_near, x_far, c_near, c_far = refs[17:21]
    out = refs[21]
    halo, last, sem = refs[22:25]
    steps = refs[25:28]
    nx, ny, nz = u0[0].shape
    _, _, first, stop = steps_of(nx)
    wait = []
    if first > WIDE:
        wait.append(pltpu.make_async_copy(rest.at[nx - WIDE - stop :], out.at[WIDE:first], sem.at[2]))
    wait.append(pltpu.make_async_copy(rest.at[: nx - WIDE - stop], out.at[stop : nx - WIDE], sem.at[3]))
    for copy in wait:
        copy.start()
    is_odd = odd("gx") == 1
    for side in (0, 1):
        flip = is_odd if side == 0 else jnp.logical_not(is_odd)
        for q, (a, k) in enumerate(LAYERS):
            main = jnp.where(flip, x_far[q], x_near[q])
            rows = jnp.where(flip, c_far[q], c_near[q])
            put = lambda v: weight(v) if a == 2 else v
            halo[side, q, :ny, :nz] = put(main)
            halo[side, q, ny:, :nz] = rows
            for t in range(5):
                at = (len(LAYERS) + t // 2, slice(None), slice(128 * (t % 2), 128 * (t % 2) + 128))
                tile = jnp.where(flip, c_far[at], c_near[at])
                halo[side, q, 8 * t : 8 * t + 8, nz:] = pltpu.roll(tile, 124 - 8 * q, 1)

    def start(a, x):
        layers = WIDE if a == 0 else WIDE - 1
        base = (0, WIDE, 2 * WIDE - 1)[a]
        if x >= nx:
            return halo[0, base + x - nx]
        if x < 0:
            return halo[1, base + layers + x]
        return whole(x, *(u0, r0, w0)[a])

    def span(side, k):
        return (nx - k, nx + SWEEPS - k) if side == 0 else (k - SWEEPS, k)

    def value(side, k, x):
        if k == 0:
            return start(0, x)
        for j, e in enumerate((k, k + 1, nx - 2 - k, nx - 1 - k)):
            if x == e:
                return ends[k - 1][j]
        return steps[k - 1][side, x - span(side, k)[0]]

    for k in range(1, SWEEPS + 1):
        for j in range(SWEEPS):
            for side in (0, 1):
                x = span(side, k)[0] + j
                near = [value(side, k - 1, x + d) for d in (-1, 0, 1)]
                new = stencil(*near, start(1, x), start(2, x))
                reach = SWEEPS - k - max(0, x - nx + 1, -x)
                if k == SWEEPS:
                    last[side, j] = new[:ny, :nz]
                elif reach > 1:
                    steps[k - 1][side, j] = new
                else:
                    steps[k - 1][side, j, :ny, :nz] = new[:ny, :nz]
                    if reach == 1:
                        steps[k - 1][side, j, ny:, :nz] = new[ny:, :nz]
                        steps[k - 1][side, j, :ny, nz:] = new[:ny, nz:]
    for side in (0, 1):
        a, b = span(side, SWEEPS)
        copy = pltpu.make_async_copy(last.at[side], out.at[a:b], sem.at[side])
        copy.start()
        wait.append(copy)
    for copy in wait:
        copy.wait()


def shards(u, r, s):
    nx, ny, nz = u.shape
    cells = nx * ny * nz
    raw = [pltpu.with_memory_space_constraint(v, pltpu.HBM) for v in (u, r, s)]
    faces = [(nx // 4, 5, 8, nz)] * 2 + [(3, nx // 32, ny, 128)] * 2 + [(len(LAYERS), ny, nz)] * 2
    scratch = [pltpu.SemaphoreType.DMA((nx // CHUNK, 3))]
    u, r, s, *sent = call(pack, [u.shape] * 3 + faces, raw, cells // 4, scratch, hbm_in=range(3))
    y = swap(sent[0:2], "gy")
    z = swap(sent[2:4], "gz")
    x = swap(sent[4:6], "gx")
    w, part, edge = call(begin, [u.shape] * 2 + [(nx, ny, 128)], (u, r, s), 20 * cells)
    sent = call(pack_yz, [(3, nx // 32, 8, 128)] * 2, z, cells // 64)
    b = swap(sent, "gy")
    t = call(unpack_z, [(nx, ny, 128)] * 3, z, 8 * cells)
    yy = call(unpack_y, [(nx, 8, nz)] * 3, y, cells)
    shape = (len(LAYERS) + 3, 8, nz)
    *e, c_near, c_far = call(pack_edges, [(nx, 8, 128)] * 3 + [shape] * 2, (*b, *yy, *t), cells // 8)
    c = swap((c_near, c_far), "gx")
    parts = [v for a, m in enumerate((u, r, w)) for v in (m, yy[a], t[a], e[a])]
    block = (ny + 2 * WIDE, nz + 128)
    _, _, first, stop = steps_of(nx)
    scratch = [pltpu.VMEM(u.shape, F32), pltpu.SemaphoreType.DMA] + [pltpu.VMEM((nx,) + block, F32)] * 3
    left = (nx - WIDE - stop + first - WIDE, ny, nz)
    out, rest, *ends = call(
        centre, [u.shape, left] + [(4,) + block] * 3, (*parts, part, edge), 60 * cells, scratch, 16, hbm_out=(0,)
    )
    scratch = [
        pltpu.VMEM((2, len(LAYERS)) + block, F32),
        pltpu.VMEM((2, WIDE, ny, nz), F32),
        pltpu.SemaphoreType.DMA((4,)),
    ] + [pltpu.VMEM((2, SWEEPS) + block, F32)] * 3
    operands = (*parts, out, rest, *ends, *x, *c)
    (out,) = call(
        tail, [u.shape], operands, 8 * cells, scratch, 8, hbm_in=(12,), hbm_out=(0,), aliases={12: 0}
    )
    return out


def solution(mesh):
    spec = P("gx", "gy", "gz")
    return jax.shard_map(shards, mesh=mesh, in_specs=(spec,) * 3, out_specs=spec, check_vma=False)
```

```python
import jax
import jax.numpy as jnp
from jax import lax
from jax.experimental import pallas as pl
from jax.experimental.pallas import tpu as pltpu
from jax.sharding import PartitionSpec as P


SWEEPS = 4
WIDE = 4
WEIGHT = 0.8
VMEM = pl.BlockSpec(memory_space=pltpu.VMEM)
HBM = pl.BlockSpec(memory_space=pltpu.HBM)
F32 = jnp.float32
CHUNK = 8
LAYERS = [(a, k) for a, n in enumerate((WIDE, WIDE - 1, WIDE - 1)) for k in range(n)]


def call(kernel, outs, operands, flops, scratch=(), limit=4, hbm_in=(), hbm_out=(), aliases={}):
    return pl.pallas_call(
        kernel,
        out_shape=[jax.ShapeDtypeStruct(s, F32) for s in outs],
        in_specs=[HBM if i in hbm_in else VMEM for i in range(len(operands))],
        out_specs=[HBM if i in hbm_out else VMEM for i in range(len(outs))],
        scratch_shapes=scratch,
        input_output_aliases=aliases,
        compiler_params=pltpu.CompilerParams(vmem_limit_bytes=limit * 2**20),
        cost_estimate=pl.CostEstimate(flops=flops, bytes_accessed=2**20, transcendentals=0),
    )(*operands)


def odd(axis):
    return lax.rem(lax.axis_index(axis), 2)


def swap(sent, axis):
    n = lax.axis_size(axis)
    near = [(i, i ^ 1) for i in range(n)]
    far = [(i, (i + (1 if i % 2 else -1)) % n) for i in range(n)]
    got = lax.ppermute(sent[1], axis, far)
    return lax.ppermute(sent[0], axis, near), got


def iota(shape, dim):
    return lax.broadcasted_iota(jnp.int32, shape, dim)


def fold(first, second, low):
    row = iota(first.shape, 0)
    keep = jnp.where(low, row, 7 - row) < 4
    return jnp.where(keep, first, pltpu.roll(second, 4, 0))


def unfold(above, below):
    head = iota(above.shape, 0) < 4
    return jnp.where(head, above, below), pltpu.roll(jnp.where(head, below, above), 4, 0)


def turn(tile, n):
    return pltpu.roll(tile, n % 8, 0) if n % 8 else tile


def fold_rows(held, x, at):
    row = iota((8, held[0].shape[2]), 0)
    tiles, rest = [], None
    for k in range(4):
        u, r, s = (ref[x + k, at : at + 8, :] for ref in held)
        if at == 0:
            tiles.append(jnp.where(row < 4, u, jnp.where(row < 7, turn(r, 4), turn(s, 7))))
            two = turn(s, 2 * k - 1)
        else:
            tiles.append(jnp.where(row > 3, u, jnp.where(row > 0, turn(r, 4), turn(s, 1))))
            two = turn(s, 2 * k - 5)
        rest = two if k == 0 else jnp.where(row // 2 == k, two, rest)
    return tiles + [rest]


def pack(u, r, s, u_v, r_v, s_v, y_near, y_far, z_near, z_far, x_near, x_far, sem):
    nx, ny, nz = u.shape
    y_odd, z_odd, x_odd = odd("gy") == 1, odd("gz") == 1, odd("gx") == 1
    held = (u_v, r_v, s_v)
    copies = {}
    for c in range(nx // CHUNK):
        at = pl.ds(c * CHUNK, CHUNK)
        for a, ref in enumerate((u, r, s)):
            copies[c, a] = pltpu.make_async_copy(ref.at[at], held[a].at[at], sem.at[c, a])
            copies[c, a].start()
    block = iota((ny, 128), 1) // 4
    half = iota((ny, 128), 1) < 64
    for c in range(nx // CHUNK):
        for a, ref in enumerate(held):
            copies[c, a].wait()
            g = c * CHUNK // 32
            first = c * CHUNK % 32 == 0
            low = jnp.zeros((ny, 128), F32) if first else z_near[a, g]
            high = jnp.zeros((ny, 128), F32) if first else z_far[a, g]
            low, high = jnp.where(z_odd, low, high), jnp.where(z_odd, high, low)
            for x in range(c * CHUNK, (c + 1) * CHUNK):
                j = x % 32
                both = jnp.where(half, ref[x, :, 0:128], ref[x, :, nz - 128 : nz])
                both = pltpu.roll(both, 4 * j, 1) if j else both
                low = jnp.where(block == j, both, low)
                high = jnp.where(block == (j - 1) % 32, both, high)
            z_near[a, g] = jnp.where(z_odd, low, high)
            z_far[a, g] = jnp.where(z_odd, high, low)
        for i in range(c * CHUNK // 4, (c + 1) * CHUNK // 4):
            low, high = fold_rows(held, 4 * i, 0), fold_rows(held, 4 * i, ny - 8)
            for n in range(5):
                y_near[i, n] = jnp.where(y_odd, low[n], high[n])
                y_far[i, n] = jnp.where(y_odd, high[n], low[n])
    for face, low in ((x_near, x_odd), (x_far, jnp.logical_not(x_odd))):
        for q, (a, k) in enumerate(LAYERS):
            layers = WIDE if a == 0 else WIDE - 1
            face[q] = held[a][jnp.where(low, k, nx - layers + k)]


def pack_yz(za, zb, near, far):
    ny = za.shape[2]
    is_odd = odd("gy") == 1
    for face, low in ((near, is_odd), (far, jnp.logical_not(is_odd))):
        rows = pl.ds(pl.multiple_of(jnp.where(low, 0, ny - 8), 8), 8)
        for a in range(3):
            for g in range(za.shape[1]):
                face[a, g] = fold(za[a, g, rows, :], zb[a, g, rows, :], low)


def weight(shift):
    return WEIGHT / (6.0 + shift)


def spread_z(high, low, j):
    tile = jnp.where(iota(high.shape, 1) // 4 == j, high, low)
    return pltpu.roll(tile, 128 - 4 * j, 1) if j else tile


def begin(u, r, s, w, part, edge):
    nx, ny, nz = u.shape
    row, lane = iota((ny, nz), 0), iota((ny, nz), 1)
    half = iota((ny, 128), 1) < 64

    def body(i, c):
        for j in range(8):
            x = 8 * i + j
            here = u[x]
            beside = u[jnp.maximum(x - 1, 0)] + u[jnp.minimum(x + 1, nx - 1)]
            beside = beside + jnp.where(row == 0, 0.0, pltpu.roll(here, 1, 0))
            beside = beside + jnp.where(row == ny - 1, 0.0, pltpu.roll(here, ny - 1, 0))
            left, right = pltpu.roll(here, 1, 1), pltpu.roll(here, nz - 1, 1)
            edge[x] = jnp.where(half, left[:, :128], right[:, nz - 128 :])
            beside = beside + (jnp.where(lane == 0, 0.0, left) + jnp.where(lane == nz - 1, 0.0, right))
            here_w = weight(s[x])
            w[x] = here_w
            part[x] = 0.2 * here + here_w * (r[x] + beside)
        return c

    lax.fori_loop(0, nx // 8, body, 0)


def finish(x, u0, r0, w0, part, edge, new):
    (u, yu, tu, eu), (_, yr, tr, er), (w, yw, tw, ew) = u0, r0, w0
    ny, nz = u.shape[1:]
    row, lane, lane_z = iota((8, nz), 0), iota((ny, 128), 1), iota((8, nz), 1)
    lane_e = iota((8, 128), 1)
    y, t, e = yu[x], tu[x], eu[x]
    t_left, t_right = pltpu.roll(t, 1, 1), pltpu.roll(t, 127, 1)
    e_left, e_right = pltpu.roll(e, 1, 1), pltpu.roll(e, 127, 1)
    y_left, y_right = pltpu.roll(y, 1, 1), pltpu.roll(y, nz - 1, 1)
    y_down, y_up = pltpu.roll(y, 1, 0), pltpu.roll(y, 7, 0)
    halo = jnp.concatenate([jnp.where(lane == 0, t_left, 0.0), jnp.where(lane == 127, t_right, 0.0)], 1)
    halo = jnp.concatenate(
        [
            halo[:8] + jnp.where(row == 0, y_down, 0.0),
            halo[8 : ny - 8],
            halo[ny - 8 :] + jnp.where(row == 7, y_up, 0.0),
        ],
        0,
    )
    new[x, :ny, :nz] = part[x] + w[x] * halo
    beside = yu[x - 1] + yu[x + 1]
    beside = beside + jnp.where(row == 0, pltpu.roll(u[x, ny - 8 :, :], 1, 0), y_down)
    beside = beside + jnp.where(row == 7, pltpu.roll(u[x, :8, :], 7, 0), y_up)
    left = jnp.where(lane_z == 0, jnp.concatenate([e_left, e_left], 1), y_left)
    right = jnp.where(lane_z == nz - 1, jnp.concatenate([e_right, e_right], 1), y_right)
    new[x, ny:, :nz] = 0.2 * y + yw[x] * (yr[x] + (beside + (left + right)))
    column = jnp.concatenate([t, e], 0)
    beside = jnp.concatenate([tu[x - 1] + tu[x + 1], eu[x - 1] + eu[x + 1]], 0)
    beside = beside + (pltpu.roll(column, 1, 0) + pltpu.roll(column, ny + 7, 0))
    left = [jnp.where(lane == 0, edge[x], t_left), jnp.where(lane_e == 0, y_left[:, :128], e_left)]
    right = [jnp.where(lane == 127, edge[x], t_right), jnp.where(lane_e == 127, y_right[:, nz - 128 :], e_right)]
    beside = beside + (jnp.concatenate(left, 0) + jnp.concatenate(right, 0))
    r, w = jnp.concatenate([tr[x], er[x]], 0), jnp.concatenate([tw[x], ew[x]], 0)
    new[x, :, nz:] = 0.2 * column + w * (r + beside)


def spread_z(high, low, j):
    tile = jnp.where(iota(high.shape, 1) // 4 == j, high, low)
    return pltpu.roll(tile, 128 - 4 * j, 1) if j else tile


def unpack_z(za, zb, tu, tr, tw):
    is_odd = odd("gz") == 1
    for a, out in enumerate((tu, tr, tw)):

        def body(g, c, a=a, out=out):
            one, two = za[a, g], zb[a, g]
            high, low = jnp.where(is_odd, two, one), jnp.where(is_odd, one, two)
            for j in range(32):
                tile = spread_z(high, low, j)
                out[g * 32 + j] = weight(tile) if a == 2 else tile
            return c

        lax.fori_loop(0, za.shape[1], body, 0)


def unpack_y(near, far, yu, yr, yw):
    is_odd = odd("gy") == 1
    row = iota(near.shape[2:], 0)

    def body(i, c):
        def halves(n):
            one, two = near[i, n], far[i, n]
            return jnp.where(is_odd, two, one), jnp.where(is_odd, one, two)

        rest_above, rest_below = halves(4)
        for k in range(4):
            above, below = halves(k)
            yu[4 * i + k] = jnp.where(row < 4, above, below)
            yr[4 * i + k] = turn(jnp.where(row < 4, below, above), 4)
            s = jnp.where(row < 4, turn(rest_above, 1 - 2 * k), turn(rest_below, 5 - 2 * k))
            s = jnp.where(row == 0, turn(above, 1), jnp.where(row == 7, turn(below, 7), s))
            yw[4 * i + k] = weight(s)
        return c

    lax.fori_loop(0, near.shape[0], body, 0, unroll=2)


def pack_edges(b_near, b_far, yu, yr, yw, tu, tr, tw, eu, er, ew, near, far):
    y_odd, z_odd, x_odd = odd("gy") == 1, odd("gz") == 1, odd("gx") == 1
    for a, out in enumerate((eu, er, ew)):
        for g in range(b_near.shape[1]):
            one, two = b_near[a, g], b_far[a, g]
            above, below = jnp.where(y_odd, two, one), jnp.where(y_odd, one, two)
            first, second = unfold(above, below)
            high, low = jnp.where(z_odd, second, first), jnp.where(z_odd, first, second)
            for j in range(32):
                tile = spread_z(high, low, j)
                out[g * 32 + j] = weight(tile) if a == 2 else tile
    nx = yu.shape[0]
    lane = iota((8, 128), 1) // 8
    for face, low in ((near, x_odd), (far, jnp.logical_not(x_odd))):
        total = [jnp.zeros((8, 128), F32)] * 5
        for q, (a, k) in enumerate(LAYERS):
            layers = WIDE if a == 0 else WIDE - 1
            x = jnp.where(low, k, nx - layers + k)
            face[q] = (yu, yr, yw)[a][x]
            for t in range(5):
                tile = (tu, tr, tw)[a][x, 8 * t : 8 * t + 8, :] if t < 4 else (eu, er, ew)[a][x]
                total[t] = jnp.where(lane == q, pltpu.roll(tile, 8 * q + 4, 1), total[t])
        for t in range(6):
            face[len(LAYERS) + t // 2, :, 128 * (t % 2) : 128 * (t % 2) + 128] = total[min(t, 4)]


def stencil(below, here, above, r, w):
    n, m = here.shape
    beside = below + above
    beside = beside + (pltpu.roll(here, 1, 0) + pltpu.roll(here, n - 1, 0))
    beside = beside + (pltpu.roll(here, 1, 1) + pltpu.roll(here, m - 1, 1))
    return 0.2 * here + w * (r + beside)


def final(below, here, above, r, w, ny, nz):
    row, lane = iota((8, nz), 0), iota((ny, 128), 1)
    tiles = [here[:ny, at : at + 128] for at in range(0, nz + 128, 128)]
    n = len(tiles)
    beside = below[:ny, :nz] + above[:ny, :nz]
    column = here[:, :nz]
    rows = column.shape[0]
    beside = beside + (pltpu.roll(column, 1, 0)[:ny] + pltpu.roll(column, rows - 1, 0)[:ny])
    left = [pltpu.roll(jnp.where(lane == 127, tiles[i - 1], tiles[i]), 1, 1) for i in range(n - 1)]
    right = [pltpu.roll(jnp.where(lane == 0, tiles[i + 1], tiles[i]), 127, 1) for i in range(n - 1)]
    beside = beside + (jnp.concatenate(left, 1) + jnp.concatenate(right, 1))
    return 0.2 * here[:ny, :nz] + w[:ny, :nz] * (r[:ny, :nz] + beside)


def whole(x, main, y, t, e):
    left = jnp.concatenate([main[x], y[x]], 0)
    return jnp.concatenate([left, jnp.concatenate([t[x], e[x]], 0)], 1)


PLANES = 4


def planes(i):
    return [(k, 1 + PLANES * i - k * (PLANES + 1) + j) for k in range(SWEEPS) for j in range(PLANES)]


def steps_of(nx):
    def valid(k, x):
        return k + 1 <= x <= nx - 2 - k

    count = -(-(nx - 1 + (SWEEPS - 1) * (PLANES + 1)) // PLANES)
    done = [[p for p in planes(i) if valid(*p)] for i in range(count)]
    full = [i for i in range(count) if len(done[i]) == SWEEPS * PLANES]
    first = planes(full[0])[-PLANES][1]
    stop = planes(full[-1])[-1][1] + 1
    return done, full, first, stop


def centre(*refs):
    u0, r0, w0 = refs[0:4], refs[4:8], refs[8:12]
    part, edge = refs[12:14]
    out, rest, ends = refs[14], refs[15], refs[16:19]
    last, sem = refs[19:21]
    steps = refs[21:24]
    nx, ny, nz = u0[0].shape
    done, full, first, stop = steps_of(nx)

    def plane(k, x):
        return steps[k - 1][x]

    def one(k, x):
        if k == 0:
            finish(x, u0, r0, w0, part, edge, steps[0])
            return
        r, w = whole(x, *r0), whole(x, *w0)
        near = plane(k, x - 1), plane(k, x), plane(k, x + 1)
        new = final(*near, r, w, ny, nz) if k == SWEEPS - 1 else stencil(*near, r, w)
        if k < SWEEPS - 2:
            steps[k][x] = new
        elif k == SWEEPS - 2:
            steps[k][x, :, :nz] = new[:, :nz]
            steps[k][x, :ny, nz:] = new[:ny, nz:]
        elif isinstance(x, int):
            rest[x - stop if x >= stop else nx - WIDE - stop + x - WIDE] = new
        else:
            last[x] = new

    for i in range(full[0]):
        for p in done[i]:
            one(*p)

    def body(i, c):
        for p in planes(i):
            one(*p)
        at = pl.ds(planes(i)[-PLANES][1], PLANES)
        pltpu.make_async_copy(last.at[at], out.at[at], sem).start()
        return c

    lax.fori_loop(full[0], full[-1] + 1, body, 0)
    for i in range(full[-1] + 1, len(done)):
        for p in done[i]:
            one(*p)
    for k in range(SWEEPS - 1):
        lo, hi = k + 1, nx - 1 - k
        for j, x in enumerate((lo, lo + 1, hi - 2, hi - 1)):
            ends[k][j] = steps[k][x]
    pltpu.make_async_copy(last.at[first:stop], out.at[first:stop], sem).wait()


def tail(*refs):
    u0, r0, w0 = refs[0:4], refs[4:8], refs[8:12]
    rest, ends = refs[13], refs[14:17]
    x_near, x_far, c_near, c_far = refs[17:21]
    out = refs[21]
    halo, last, sem = refs[22:25]
    steps = refs[25:28]
    nx, ny, nz = u0[0].shape
    _, _, first, stop = steps_of(nx)
    wait = []
    if first > WIDE:
        wait.append(pltpu.make_async_copy(rest.at[nx - WIDE - stop :], out.at[WIDE:first], sem.at[2]))
    wait.append(pltpu.make_async_copy(rest.at[: nx - WIDE - stop], out.at[stop : nx - WIDE], sem.at[3]))
    for copy in wait:
        copy.start()
    is_odd = odd("gx") == 1
    for side in (0, 1):
        flip = is_odd if side == 0 else jnp.logical_not(is_odd)
        for q, (a, k) in enumerate(LAYERS):
            main = jnp.where(flip, x_far[q], x_near[q])
            rows = jnp.where(flip, c_far[q], c_near[q])
            put = lambda v: weight(v) if a == 2 else v
            halo[side, q, :ny, :nz] = put(main)
            halo[side, q, ny:, :nz] = rows
            for t in range(5):
                at = (len(LAYERS) + t // 2, slice(None), slice(128 * (t % 2), 128 * (t % 2) + 128))
                tile = jnp.where(flip, c_far[at], c_near[at])
                halo[side, q, 8 * t : 8 * t + 8, nz:] = pltpu.roll(tile, 124 - 8 * q, 1)

    def start(a, x):
        layers = WIDE if a == 0 else WIDE - 1
        base = (0, WIDE, 2 * WIDE - 1)[a]
        if x >= nx:
            return halo[0, base + x - nx]
        if x < 0:
            return halo[1, base + layers + x]
        return whole(x, *(u0, r0, w0)[a])

    def span(side, k):
        return (nx - k, nx + SWEEPS - k) if side == 0 else (k - SWEEPS, k)

    def value(side, k, x):
        if k == 0:
            return start(0, x)
        for j, e in enumerate((k, k + 1, nx - 2 - k, nx - 1 - k)):
            if x == e:
                return ends[k - 1][j]
        return steps[k - 1][side, x - span(side, k)[0]]

    for k in range(1, SWEEPS + 1):
        for j in range(SWEEPS):
            for side in (0, 1):
                x = span(side, k)[0] + j
                near = [value(side, k - 1, x + d) for d in (-1, 0, 1)]
                coefficients = start(1, x), start(2, x)
                reach = SWEEPS - k - max(0, x - nx + 1, -x)
                if reach == 0:
                    new = final(*near, *coefficients, ny, nz)
                    if k == SWEEPS:
                        last[side, j] = new
                    else:
                        steps[k - 1][side, j, :ny, :nz] = new
                    continue
                new = stencil(*near, *coefficients)
                if reach > 1:
                    steps[k - 1][side, j] = new
                else:
                    steps[k - 1][side, j, :, :nz] = new[:, :nz]
                    steps[k - 1][side, j, :ny, nz:] = new[:ny, nz:]
    for side in (0, 1):
        a, b = span(side, SWEEPS)
        copy = pltpu.make_async_copy(last.at[side], out.at[a:b], sem.at[side])
        copy.start()
        wait.append(copy)
    for copy in wait:
        copy.wait()


def shards(u, r, s):
    nx, ny, nz = u.shape
    cells = nx * ny * nz
    raw = [pltpu.with_memory_space_constraint(v, pltpu.HBM) for v in (u, r, s)]
    faces = [(nx // 4, 5, 8, nz)] * 2 + [(3, nx // 32, ny, 128)] * 2 + [(len(LAYERS), ny, nz)] * 2
    scratch = [pltpu.SemaphoreType.DMA((nx // CHUNK, 3))]
    u, r, s, *sent = call(pack, [u.shape] * 3 + faces, raw, cells // 4, scratch, hbm_in=range(3))
    y = swap(sent[0:2], "gy")
    z = swap(sent[2:4], "gz")
    x = swap(sent[4:6], "gx")
    w, part, edge = call(begin, [u.shape] * 2 + [(nx, ny, 128)], (u, r, s), 20 * cells)
    sent = call(pack_yz, [(3, nx // 32, 8, 128)] * 2, z, cells // 64)
    b = swap(sent, "gy")
    t = call(unpack_z, [(nx, ny, 128)] * 3, z, 8 * cells)
    yy = call(unpack_y, [(nx, 8, nz)] * 3, y, cells)
    shape = (len(LAYERS) + 3, 8, nz)
    *e, c_near, c_far = call(pack_edges, [(nx, 8, 128)] * 3 + [shape] * 2, (*b, *yy, *t), cells // 8)
    c = swap((c_near, c_far), "gx")
    parts = [v for a, m in enumerate((u, r, w)) for v in (m, yy[a], t[a], e[a])]
    block = (ny + 2 * WIDE, nz + 128)
    _, _, first, stop = steps_of(nx)
    scratch = [pltpu.VMEM(u.shape, F32), pltpu.SemaphoreType.DMA] + [pltpu.VMEM((nx,) + block, F32)] * 3
    left = (nx - WIDE - stop + first - WIDE, ny, nz)
    out, rest, *ends = call(
        centre, [u.shape, left] + [(4,) + block] * 3, (*parts, part, edge), 60 * cells, scratch, 16, hbm_out=(0,)
    )
    scratch = [
        pltpu.VMEM((2, len(LAYERS)) + block, F32),
        pltpu.VMEM((2, WIDE, ny, nz), F32),
        pltpu.SemaphoreType.DMA((4,)),
    ] + [pltpu.VMEM((2, SWEEPS) + block, F32)] * 3
    operands = (*parts, out, rest, *ends, *x, *c)
    (out,) = call(
        tail, [u.shape], operands, 8 * cells, scratch, 8, hbm_in=(12,), hbm_out=(0,), aliases={12: 0}
    )
    return out


def solution(mesh):
    spec = P("gx", "gy", "gz")
    return jax.shard_map(shards, mesh=mesh, in_specs=(spec,) * 3, out_specs=spec, check_vma=False)
```

```python
import jax
import jax.numpy as jnp
from jax import lax
from jax.experimental import pallas as pl
from jax.experimental.pallas import tpu as pltpu
from jax.sharding import PartitionSpec as P


SWEEPS = 4
WIDE = 4
WEIGHT = 0.8
VMEM = pl.BlockSpec(memory_space=pltpu.VMEM)
HBM = pl.BlockSpec(memory_space=pltpu.HBM)
F32 = jnp.float32
LAYERS = [(a, k) for a, n in enumerate((WIDE, WIDE - 1, WIDE - 1)) for k in range(n)]


def call(kernel, outs, operands, flops, scratch=(), limit=4, hbm_in=(), hbm_out=(), aliases={}):
    return pl.pallas_call(
        kernel,
        out_shape=[jax.ShapeDtypeStruct(s, F32) for s in outs],
        in_specs=[HBM if i in hbm_in else VMEM for i in range(len(operands))],
        out_specs=[HBM if i in hbm_out else VMEM for i in range(len(outs))],
        scratch_shapes=scratch,
        input_output_aliases=aliases,
        compiler_params=pltpu.CompilerParams(vmem_limit_bytes=limit * 2**20),
        cost_estimate=pl.CostEstimate(flops=flops, bytes_accessed=2**20, transcendentals=0),
    )(*operands)


def odd(axis):
    return lax.rem(lax.axis_index(axis), 2)


def swap(sent, axis):
    n = lax.axis_size(axis)
    near = [(i, i ^ 1) for i in range(n)]
    far = [(i, (i + (1 if i % 2 else -1)) % n) for i in range(n)]
    got = lax.ppermute(sent[1], axis, far)
    return lax.ppermute(sent[0], axis, near), got


def iota(shape, dim):
    return lax.broadcasted_iota(jnp.int32, shape, dim)


def fold(first, second, low):
    row = iota(first.shape, 0)
    keep = jnp.where(low, row, 7 - row) < 4
    return jnp.where(keep, first, pltpu.roll(second, 4, 0))


def unfold(above, below):
    head = iota(above.shape, 0) < 4
    return jnp.where(head, above, below), pltpu.roll(jnp.where(head, below, above), 4, 0)


def chunks(nx):
    sizes = [32] * (nx // 32 - 1) + [16, 16]
    return [(sum(sizes[:i]), n) for i, n in enumerate(sizes)]


def turn(tile, n):
    return pltpu.roll(tile, n % 8, 0) if n % 8 else tile


def fold_rows(held, x, at):
    row = iota((8, held[0].shape[2]), 0)
    tiles, rest = [], None
    for k in range(4):
        u, r, s = (ref[x + k, at : at + 8, :] for ref in held)
        if at == 0:
            tiles.append(jnp.where(row < 4, u, jnp.where(row < 7, turn(r, 4), turn(s, 7))))
            two = turn(s, 2 * k - 1)
        else:
            tiles.append(jnp.where(row > 3, u, jnp.where(row > 0, turn(r, 4), turn(s, 1))))
            two = turn(s, 2 * k - 5)
        rest = two if k == 0 else jnp.where(row // 2 == k, two, rest)
    return tiles + [rest]


def pack(u, r, s, u_v, r_v, s_v, y_near, y_far, z_near, z_far, x_near, x_far, sem):
    nx, ny, nz = u.shape
    y_odd, z_odd, x_odd = odd("gy") == 1, odd("gz") == 1, odd("gx") == 1
    held = (u_v, r_v, s_v)
    copies = {}
    for c, (x0, size) in enumerate(chunks(nx)):
        at = pl.ds(x0, size)
        for a, ref in enumerate((u, r, s)):
            copies[c, a] = pltpu.make_async_copy(ref.at[at], held[a].at[at], sem.at[c, a])
            copies[c, a].start()
    block = iota((ny, 128), 1) // 4
    half = iota((ny, 128), 1) < 64
    for c, (x0, size) in enumerate(chunks(nx)):
        for a, ref in enumerate(held):
            copies[c, a].wait()
            g = x0 // 32
            first = x0 % 32 == 0
            low = jnp.zeros((ny, 128), F32) if first else z_near[a, g]
            high = jnp.zeros((ny, 128), F32) if first else z_far[a, g]
            low, high = jnp.where(z_odd, low, high), jnp.where(z_odd, high, low)
            for x in range(x0, x0 + size):
                j = x % 32
                both = jnp.where(half, ref[x, :, 0:128], ref[x, :, nz - 128 : nz])
                both = pltpu.roll(both, 4 * j, 1) if j else both
                low = jnp.where(block == j, both, low)
                high = jnp.where(block == (j - 1) % 32, both, high)
            z_near[a, g] = jnp.where(z_odd, low, high)
            z_far[a, g] = jnp.where(z_odd, high, low)
        for i in range(x0 // 4, (x0 + size) // 4):
            low, high = fold_rows(held, 4 * i, 0), fold_rows(held, 4 * i, ny - 8)
            for n in range(5):
                y_near[i, n] = jnp.where(y_odd, low[n], high[n])
                y_far[i, n] = jnp.where(y_odd, high[n], low[n])
    for face, low in ((x_near, x_odd), (x_far, jnp.logical_not(x_odd))):
        for q, (a, k) in enumerate(LAYERS):
            layers = WIDE if a == 0 else WIDE - 1
            face[q] = held[a][jnp.where(low, k, nx - layers + k)]


def pack_yz(za, zb, near, far):
    ny = za.shape[2]
    is_odd = odd("gy") == 1
    for face, low in ((near, is_odd), (far, jnp.logical_not(is_odd))):
        rows = pl.ds(pl.multiple_of(jnp.where(low, 0, ny - 8), 8), 8)
        for a in range(3):
            for g in range(za.shape[1]):
                face[a, g] = fold(za[a, g, rows, :], zb[a, g, rows, :], low)


def weight(shift):
    return WEIGHT / (6.0 + shift)


def spread_z(high, low, j):
    tile = jnp.where(iota(high.shape, 1) // 4 == j, high, low)
    return pltpu.roll(tile, 128 - 4 * j, 1) if j else tile


def begin(u, r, s, w, part, edge):
    nx, ny, nz = u.shape
    row, lane = iota((ny, nz), 0), iota((ny, nz), 1)
    half = iota((ny, 128), 1) < 64

    def body(i, c):
        for j in range(8):
            x = 8 * i + j
            here = u[x]
            beside = u[jnp.maximum(x - 1, 0)] + u[jnp.minimum(x + 1, nx - 1)]
            beside = beside + jnp.where(row == 0, 0.0, pltpu.roll(here, 1, 0))
            beside = beside + jnp.where(row == ny - 1, 0.0, pltpu.roll(here, ny - 1, 0))
            left, right = pltpu.roll(here, 1, 1), pltpu.roll(here, nz - 1, 1)
            edge[x] = jnp.where(half, left[:, :128], right[:, nz - 128 :])
            beside = beside + (jnp.where(lane == 0, 0.0, left) + jnp.where(lane == nz - 1, 0.0, right))
            here_w = weight(s[x])
            w[x] = here_w
            part[x] = 0.2 * here + here_w * (r[x] + beside)
        return c

    lax.fori_loop(0, nx // 8, body, 0)


def finish(x, u0, r0, w0, part, edge, new):
    (u, yu, tu, eu), (_, yr, tr, er), (w, yw, tw, ew) = u0, r0, w0
    ny, nz = u.shape[1:]
    row, lane, lane_z = iota((8, nz), 0), iota((ny, 128), 1), iota((8, nz), 1)
    lane_e = iota((8, 128), 1)
    y, t, e = yu[x], tu[x], eu[x]
    t_left, t_right = pltpu.roll(t, 1, 1), pltpu.roll(t, 127, 1)
    e_left, e_right = pltpu.roll(e, 1, 1), pltpu.roll(e, 127, 1)
    y_left, y_right = pltpu.roll(y, 1, 1), pltpu.roll(y, nz - 1, 1)
    y_down, y_up = pltpu.roll(y, 1, 0), pltpu.roll(y, 7, 0)
    halo = jnp.concatenate([jnp.where(lane == 0, t_left, 0.0), jnp.where(lane == 127, t_right, 0.0)], 1)
    halo = jnp.concatenate(
        [
            halo[:8] + jnp.where(row == 0, y_down, 0.0),
            halo[8 : ny - 8],
            halo[ny - 8 :] + jnp.where(row == 7, y_up, 0.0),
        ],
        0,
    )
    new[x, :ny, :nz] = part[x] + w[x] * halo
    beside = yu[x - 1] + yu[x + 1]
    beside = beside + jnp.where(row == 0, pltpu.roll(u[x, ny - 8 :, :], 1, 0), y_down)
    beside = beside + jnp.where(row == 7, pltpu.roll(u[x, :8, :], 7, 0), y_up)
    left = jnp.where(lane_z == 0, jnp.concatenate([e_left, e_left], 1), y_left)
    right = jnp.where(lane_z == nz - 1, jnp.concatenate([e_right, e_right], 1), y_right)
    new[x, ny:, :nz] = 0.2 * y + yw[x] * (yr[x] + (beside + (left + right)))
    column = jnp.concatenate([t, e], 0)
    beside = jnp.concatenate([tu[x - 1] + tu[x + 1], eu[x - 1] + eu[x + 1]], 0)
    beside = beside + (pltpu.roll(column, 1, 0) + pltpu.roll(column, ny + 7, 0))
    left = [jnp.where(lane == 0, edge[x], t_left), jnp.where(lane_e == 0, y_left[:, :128], e_left)]
    right = [jnp.where(lane == 127, edge[x], t_right), jnp.where(lane_e == 127, y_right[:, nz - 128 :], e_right)]
    beside = beside + (jnp.concatenate(left, 0) + jnp.concatenate(right, 0))
    r, w = jnp.concatenate([tr[x], er[x]], 0), jnp.concatenate([tw[x], ew[x]], 0)
    new[x, :, nz:] = 0.2 * column + w * (r + beside)


def spread_z(high, low, j):
    tile = jnp.where(iota(high.shape, 1) // 4 == j, high, low)
    return pltpu.roll(tile, 128 - 4 * j, 1) if j else tile


def unpack_z(za, zb, tu, tr, tw):
    is_odd = odd("gz") == 1
    for a, out in enumerate((tu, tr, tw)):

        def body(g, c, a=a, out=out):
            one, two = za[a, g], zb[a, g]
            high, low = jnp.where(is_odd, two, one), jnp.where(is_odd, one, two)
            for j in range(32):
                tile = spread_z(high, low, j)
                out[g * 32 + j] = weight(tile) if a == 2 else tile
            return c

        lax.fori_loop(0, za.shape[1], body, 0)


def unpack_y(near, far, yu, yr, yw):
    is_odd = odd("gy") == 1
    row = iota(near.shape[2:], 0)

    def body(i, c):
        def halves(n):
            one, two = near[i, n], far[i, n]
            return jnp.where(is_odd, two, one), jnp.where(is_odd, one, two)

        rest_above, rest_below = halves(4)
        for k in range(4):
            above, below = halves(k)
            yu[4 * i + k] = jnp.where(row < 4, above, below)
            yr[4 * i + k] = turn(jnp.where(row < 4, below, above), 4)
            s = jnp.where(row < 4, turn(rest_above, 1 - 2 * k), turn(rest_below, 5 - 2 * k))
            s = jnp.where(row == 0, turn(above, 1), jnp.where(row == 7, turn(below, 7), s))
            yw[4 * i + k] = weight(s)
        return c

    lax.fori_loop(0, near.shape[0], body, 0, unroll=2)


def pack_edges(b_near, b_far, yu, yr, yw, tu, tr, tw, eu, er, ew, near, far):
    y_odd, z_odd, x_odd = odd("gy") == 1, odd("gz") == 1, odd("gx") == 1
    for a, out in enumerate((eu, er, ew)):
        for g in range(b_near.shape[1]):
            one, two = b_near[a, g], b_far[a, g]
            above, below = jnp.where(y_odd, two, one), jnp.where(y_odd, one, two)
            first, second = unfold(above, below)
            high, low = jnp.where(z_odd, second, first), jnp.where(z_odd, first, second)
            for j in range(32):
                tile = spread_z(high, low, j)
                out[g * 32 + j] = weight(tile) if a == 2 else tile
    nx = yu.shape[0]
    lane = iota((8, 128), 1) // 8
    for face, low in ((near, x_odd), (far, jnp.logical_not(x_odd))):
        total = [jnp.zeros((8, 128), F32)] * 5
        for q, (a, k) in enumerate(LAYERS):
            layers = WIDE if a == 0 else WIDE - 1
            x = jnp.where(low, k, nx - layers + k)
            face[q] = (yu, yr, yw)[a][x]
            for t in range(5):
                tile = (tu, tr, tw)[a][x, 8 * t : 8 * t + 8, :] if t < 4 else (eu, er, ew)[a][x]
                total[t] = jnp.where(lane == q, pltpu.roll(tile, 8 * q + 4, 1), total[t])
        for t in range(6):
            face[len(LAYERS) + t // 2, :, 128 * (t % 2) : 128 * (t % 2) + 128] = total[min(t, 4)]


def stencil(below, here, above, r, w):
    n, m = here.shape
    beside = below + above
    beside = beside + (pltpu.roll(here, 1, 0) + pltpu.roll(here, n - 1, 0))
    beside = beside + (pltpu.roll(here, 1, 1) + pltpu.roll(here, m - 1, 1))
    return 0.2 * here + w * (r + beside)


def final(below, here, above, r, w, ny, nz):
    row, lane = iota((8, nz), 0), iota((ny, 128), 1)
    tiles = [here[:ny, at : at + 128] for at in range(0, nz + 128, 128)]
    n = len(tiles)
    beside = below[:ny, :nz] + above[:ny, :nz]
    column = here[:, :nz]
    rows = column.shape[0]
    beside = beside + (pltpu.roll(column, 1, 0)[:ny] + pltpu.roll(column, rows - 1, 0)[:ny])
    left = [pltpu.roll(jnp.where(lane == 127, tiles[i - 1], tiles[i]), 1, 1) for i in range(n - 1)]
    right = [pltpu.roll(jnp.where(lane == 0, tiles[i + 1], tiles[i]), 127, 1) for i in range(n - 1)]
    beside = beside + (jnp.concatenate(left, 1) + jnp.concatenate(right, 1))
    return 0.2 * here[:ny, :nz] + w[:ny, :nz] * (r[:ny, :nz] + beside)


def whole(x, main, y, t, e):
    left = jnp.concatenate([main[x], y[x]], 0)
    return jnp.concatenate([left, jnp.concatenate([t[x], e[x]], 0)], 1)


PLANES = 4


def planes(i):
    return [(k, 1 + PLANES * i - k * (PLANES + 1) + j) for k in range(SWEEPS) for j in range(PLANES)]


def steps_of(nx):
    def valid(k, x):
        return k + 1 <= x <= nx - 2 - k

    count = -(-(nx - 1 + (SWEEPS - 1) * (PLANES + 1)) // PLANES)
    done = [[p for p in planes(i) if valid(*p)] for i in range(count)]
    full = [i for i in range(count) if len(done[i]) == SWEEPS * PLANES]
    first = planes(full[0])[-PLANES][1]
    stop = planes(full[-1])[-1][1] + 1
    return done, full, first, stop


def centre(*refs):
    u0, r0, w0 = refs[0:4], refs[4:8], refs[8:12]
    part, edge = refs[12:14]
    out, rest, ends = refs[14], refs[15], refs[16:19]
    last, sem = refs[19:21]
    steps = refs[21:24]
    nx, ny, nz = u0[0].shape
    done, full, first, stop = steps_of(nx)

    def plane(k, x):
        return steps[k - 1][x]

    def one(k, x):
        if k == 0:
            finish(x, u0, r0, w0, part, edge, steps[0])
            return
        r, w = whole(x, *r0), whole(x, *w0)
        near = plane(k, x - 1), plane(k, x), plane(k, x + 1)
        new = final(*near, r, w, ny, nz) if k == SWEEPS - 1 else stencil(*near, r, w)
        if k < SWEEPS - 2:
            steps[k][x] = new
        elif k == SWEEPS - 2:
            steps[k][x, :, :nz] = new[:, :nz]
            steps[k][x, :ny, nz:] = new[:ny, nz:]
        elif isinstance(x, int):
            rest[x - stop if x >= stop else nx - WIDE - stop + x - WIDE] = new
        else:
            last[x] = new

    for i in range(full[0]):
        for p in done[i]:
            one(*p)

    def body(i, c):
        for p in planes(i):
            one(*p)
        at = pl.ds(planes(i)[-PLANES][1], PLANES)
        pltpu.make_async_copy(last.at[at], out.at[at], sem).start()
        return c

    lax.fori_loop(full[0], full[-1] + 1, body, 0)
    for i in range(full[-1] + 1, len(done)):
        for p in done[i]:
            one(*p)
    for k in range(SWEEPS - 1):
        lo, hi = k + 1, nx - 1 - k
        for j, x in enumerate((lo, lo + 1, hi - 2, hi - 1)):
            ends[k][j] = steps[k][x]
    pltpu.make_async_copy(last.at[first:stop], out.at[first:stop], sem).wait()


def tail(*refs):
    u0, r0, w0 = refs[0:4], refs[4:8], refs[8:12]
    rest, ends = refs[13], refs[14:17]
    x_near, x_far, c_near, c_far = refs[17:21]
    out = refs[21]
    halo, last, sem = refs[22:25]
    steps = refs[25:28]
    nx, ny, nz = u0[0].shape
    _, _, first, stop = steps_of(nx)
    wait = []
    if first > WIDE:
        wait.append(pltpu.make_async_copy(rest.at[nx - WIDE - stop :], out.at[WIDE:first], sem.at[2]))
    wait.append(pltpu.make_async_copy(rest.at[: nx - WIDE - stop], out.at[stop : nx - WIDE], sem.at[3]))
    for copy in wait:
        copy.start()
    is_odd = odd("gx") == 1
    for side in (0, 1):
        flip = is_odd if side == 0 else jnp.logical_not(is_odd)
        for q, (a, k) in enumerate(LAYERS):
            main = jnp.where(flip, x_far[q], x_near[q])
            rows = jnp.where(flip, c_far[q], c_near[q])
            put = lambda v: weight(v) if a == 2 else v
            halo[side, q, :ny, :nz] = put(main)
            halo[side, q, ny:, :nz] = rows
            for t in range(5):
                at = (len(LAYERS) + t // 2, slice(None), slice(128 * (t % 2), 128 * (t % 2) + 128))
                tile = jnp.where(flip, c_far[at], c_near[at])
                halo[side, q, 8 * t : 8 * t + 8, nz:] = pltpu.roll(tile, 124 - 8 * q, 1)

    def start(a, x):
        layers = WIDE if a == 0 else WIDE - 1
        base = (0, WIDE, 2 * WIDE - 1)[a]
        if x >= nx:
            return halo[0, base + x - nx]
        if x < 0:
            return halo[1, base + layers + x]
        return whole(x, *(u0, r0, w0)[a])

    def span(side, k):
        return (nx - k, nx + SWEEPS - k) if side == 0 else (k - SWEEPS, k)

    def value(side, k, x):
        if k == 0:
            return start(0, x)
        for j, e in enumerate((k, k + 1, nx - 2 - k, nx - 1 - k)):
            if x == e:
                return ends[k - 1][j]
        return steps[k - 1][side, x - span(side, k)[0]]

    for k in range(1, SWEEPS + 1):
        for j in range(SWEEPS):
            for side in (0, 1):
                x = span(side, k)[0] + j
                near = [value(side, k - 1, x + d) for d in (-1, 0, 1)]
                coefficients = start(1, x), start(2, x)
                reach = SWEEPS - k - max(0, x - nx + 1, -x)
                if reach == 0:
                    new = final(*near, *coefficients, ny, nz)
                    if k == SWEEPS:
                        last[side, j] = new
                    else:
                        steps[k - 1][side, j, :ny, :nz] = new
                    continue
                new = stencil(*near, *coefficients)
                if reach > 1:
                    steps[k - 1][side, j] = new
                else:
                    steps[k - 1][side, j, :, :nz] = new[:, :nz]
                    steps[k - 1][side, j, :ny, nz:] = new[:ny, nz:]
    for side in (0, 1):
        a, b = span(side, SWEEPS)
        copy = pltpu.make_async_copy(last.at[side], out.at[a:b], sem.at[side])
        copy.start()
        wait.append(copy)
    for copy in wait:
        copy.wait()


def shards(u, r, s):
    nx, ny, nz = u.shape
    cells = nx * ny * nz
    raw = [pltpu.with_memory_space_constraint(v, pltpu.HBM) for v in (u, r, s)]
    faces = [(nx // 4, 5, 8, nz)] * 2 + [(3, nx // 32, ny, 128)] * 2 + [(len(LAYERS), ny, nz)] * 2
    scratch = [pltpu.SemaphoreType.DMA((len(chunks(nx)), 3))]
    u, r, s, *sent = call(pack, [u.shape] * 3 + faces, raw, cells // 4, scratch, hbm_in=range(3))
    y = swap(sent[0:2], "gy")
    z = swap(sent[2:4], "gz")
    x = swap(sent[4:6], "gx")
    w, part, edge = call(begin, [u.shape] * 2 + [(nx, ny, 128)], (u, r, s), 20 * cells)
    sent = call(pack_yz, [(3, nx // 32, 8, 128)] * 2, z, cells // 64)
    b = swap(sent, "gy")
    t = call(unpack_z, [(nx, ny, 128)] * 3, z, 8 * cells)
    yy = call(unpack_y, [(nx, 8, nz)] * 3, y, cells)
    shape = (len(LAYERS) + 3, 8, nz)
    *e, c_near, c_far = call(pack_edges, [(nx, 8, 128)] * 3 + [shape] * 2, (*b, *yy, *t), cells // 8)
    c = swap((c_near, c_far), "gx")
    parts = [v for a, m in enumerate((u, r, w)) for v in (m, yy[a], t[a], e[a])]
    block = (ny + 2 * WIDE, nz + 128)
    _, _, first, stop = steps_of(nx)
    scratch = [pltpu.VMEM(u.shape, F32), pltpu.SemaphoreType.DMA] + [pltpu.VMEM((nx,) + block, F32)] * 3
    left = (nx - WIDE - stop + first - WIDE, ny, nz)
    out, rest, *ends = call(
        centre, [u.shape, left] + [(4,) + block] * 3, (*parts, part, edge), 60 * cells, scratch, 16, hbm_out=(0,)
    )
    scratch = [
        pltpu.VMEM((2, len(LAYERS)) + block, F32),
        pltpu.VMEM((2, WIDE, ny, nz), F32),
        pltpu.SemaphoreType.DMA((4,)),
    ] + [pltpu.VMEM((2, SWEEPS) + block, F32)] * 3
    operands = (*parts, out, rest, *ends, *x, *c)
    (out,) = call(
        tail, [u.shape], operands, 8 * cells, scratch, 8, hbm_in=(12,), hbm_out=(0,), aliases={12: 0}
    )
    return out


def solution(mesh):
    spec = P("gx", "gy", "gz")
    return jax.shard_map(shards, mesh=mesh, in_specs=(spec,) * 3, out_specs=spec, check_vma=False)
```
